8 devices in a mesh: data: 2 (over z, y), seq: 4 (over x, core).
Axes of the slice: x: 2, y: 2, z: 1, core: 2. Of those that a mesh axis runs over, the one named last changes fastest.
Arguments:
- act_in: bfloat16 [8, 1024, 1024], P('data', 'seq'), parts along dimension 0
- ln1_scale: float32 [1024], replicated
- ln1_bias: float32 [1024], replicated
- w_in: bfloat16 [1024, 6144], replicated
- b_in: float32 [6144], replicated
- ln2_scale: float32 [3072], replicated
- ln2_bias: float32 [3072], replicated
- w_spatial: bfloat16 [1024, 1024], replicated
- b_spatial: float32 [1024], replicated
- causal_mask: int32 [1024, 1024], replicated
- w_out: bfloat16 [3072, 1024], replicated
- b_out: float32 [1024], replicated
Outputs:
- output: bfloat16 [8, 1024, 1024], P('data', 'seq'), parts along dimension 0
There are 2 independent parts. The reference program is written for one: setup_inputs(seed, part) draws one part's arguments, and reference() takes and returns one part's arrays. A program takes and returns all parts, laid end to end along the dimension named above; an argument that names none is the same for every part.
All inputs are finite; a program needn't handle non-finite values.
Results may differ from the reference program's by a relative error of at most 0.0115622.
Values are sent between devices in bfloat16 or wider.
A program may use at most 1 GiB of HBM per device.

```python
import jax
import jax.numpy as jnp
from jax import lax

BATCH_ROWS = 4
SEQ_LEN = 1024
MODEL_DIM = 1024
FFN_DIM = 6144
GATE_DIM = FFN_DIM // 2
LN_EPS = 1e-6


def layer_norm(features, ln_gain, ln_shift):
    mean_val = jnp.mean(features, axis=-1, keepdims=True)
    centered = features - mean_val
    var_val = jnp.mean(centered * centered, axis=-1, keepdims=True)
    return centered * lax.rsqrt(var_val + LN_EPS) * ln_gain + ln_shift


def draw_mask(mask_key):
    cut_points = jax.random.randint(mask_key, (2,), 1, SEQ_LEN)
    positions = jnp.arange(SEQ_LEN)
    doc_id = jnp.sum(positions[:, None] >= cut_points[None, :], axis=1)
    keep_mask = (positions[None, :] <= positions[:, None]) & (doc_id[None, :] == doc_id[:, None])
    return keep_mask.astype(jnp.int32)


def setup_inputs(seed: int = 0, part: int = 0) -> dict:
    key_list = jax.random.split(jax.random.key(seed), 12)
    x_key = jax.random.fold_in(key_list[0], part)
    causal_mask = draw_mask(key_list[7])
    row_count = jnp.sum(causal_mask, axis=1).astype(jnp.float32)
    act_in = jax.random.normal(x_key, (BATCH_ROWS, SEQ_LEN, MODEL_DIM), jnp.float32)
    ln1_scale = 1.0 + 0.5 * jax.random.normal(key_list[1], (MODEL_DIM,), jnp.float32)
    ln1_bias = 0.5 * jax.random.normal(key_list[2], (MODEL_DIM,), jnp.float32)
    w_in = jax.random.normal(key_list[3], (MODEL_DIM, FFN_DIM), jnp.float32) * MODEL_DIM ** -0.5
    b_in = 0.5 * jax.random.normal(key_list[4], (FFN_DIM,), jnp.float32)
    ln2_scale = 1.0 + 0.5 * jax.random.normal(key_list[5], (GATE_DIM,), jnp.float32)
    ln2_bias = 0.5 * jax.random.normal(key_list[6], (GATE_DIM,), jnp.float32)
    w_spatial = jax.random.normal(key_list[8], (SEQ_LEN, SEQ_LEN), jnp.float32) * lax.rsqrt(row_count)[:, None]
    b_spatial = 1.0 + 0.8 * jax.random.normal(key_list[9], (SEQ_LEN,), jnp.float32)
    w_out = jax.random.normal(key_list[10], (GATE_DIM, MODEL_DIM), jnp.float32) * (2.0 * GATE_DIM ** -0.5)
    b_out = 0.3 * jax.random.normal(key_list[11], (MODEL_DIM,), jnp.float32)
    return dict(
        act_in=act_in.astype(jnp.bfloat16),
        ln1_scale=ln1_scale,
        ln1_bias=ln1_bias,
        w_in=w_in.astype(jnp.bfloat16),
        b_in=b_in,
        ln2_scale=ln2_scale,
        ln2_bias=ln2_bias,
        w_spatial=w_spatial.astype(jnp.bfloat16),
        b_spatial=b_spatial,
        causal_mask=causal_mask,
        w_out=w_out.astype(jnp.bfloat16),
        b_out=b_out,
    )


def reference(act_in, ln1_scale, ln1_bias, w_in, b_in, ln2_scale, ln2_bias, w_spatial, b_spatial, causal_mask, w_out, b_out):
    w_masked = jnp.where(causal_mask > 0, w_spatial, jnp.zeros_like(w_spatial))

    def one_sequence(seq_act):
        normed = layer_norm(seq_act.astype(jnp.float32), ln1_scale, ln1_bias).astype(jnp.bfloat16)
        hidden = jax.nn.gelu(jnp.dot(normed, w_in, preferred_element_type=jnp.float32) + b_in, approximate=True).astype(jnp.bfloat16)
        gate_half = hidden[:, :GATE_DIM]
        value_norm = layer_norm(hidden[:, GATE_DIM:].astype(jnp.float32), ln2_scale, ln2_bias).astype(jnp.bfloat16)
        spatial = (jnp.dot(w_masked, value_norm, preferred_element_type=jnp.float32) + b_spatial[:, None]).astype(jnp.bfloat16)
        gated_act = (gate_half.astype(jnp.float32) * spatial.astype(jnp.float32)).astype(jnp.bfloat16)
        projected = jnp.dot(gated_act, w_out, preferred_element_type=jnp.float32) + b_out
        return (seq_act.astype(jnp.float32) + projected).astype(jnp.bfloat16)

    return lax.map(one_sequence, act_in)
```

```python
import functools

import jax
import jax.numpy as jnp
from jax import lax
from jax.experimental import pallas as pl
from jax.experimental.pallas import tpu as pltpu
from jax.sharding import PartitionSpec as P

LN_EPS = 1e-6
GELU_A = 0.7978845608028654
GELU_B = GELU_A * 0.044715
COLS = 512
MESH = pl.DeviceIdType.MESH
F32 = jnp.float32
BF16 = jnp.bfloat16


def gelu(a):
    half = 0.5 * a
    return half + half * jnp.tanh(a * (GELU_A + GELU_B * (a * a)))


def layer_norm(x, gain, shift):
    width = x.shape[-1]
    mean = jnp.sum(x, axis=-1, keepdims=True) * (1.0 / width)
    centered = x - mean
    var = jnp.sum(centered * centered, axis=-1, keepdims=True) * (1.0 / width)
    return centered * lax.rsqrt(var + LN_EPS) * gain + shift


def body(n, act, ln1s, ln1b, w_in, b_in, ln2s, ln2b, w_sp, b_sp, mask, w_out, b_out, out,
         xbuf, wi, wo, ws, mk, vn, g, u, q, ybuf, bias,
         xs_sem, xr_sem, ys_sem, yr_sem, wi_sem, wo_sem, ws_sem, mk_sem):
    me = lax.axis_index("seq")
    chip, core = me // 2, lax.rem(me, 2)
    partner = chip * 2 + 1 - core
    far = (1 - chip) * 2
    rows, width = act.shape[1], act.shape[2]
    gate = w_out.shape[0]
    n_cols = gate // COLS

    def wi_copy(c):
        cols = pl.ds(c * COLS, COLS)
        return pltpu.make_async_copy(w_in.at[:, cols], wi.at[:, cols], wi_sem.at[c])

    def ws_copy(i):
        where = (pl.ds(i * rows, rows), pl.ds(0, (i + 1) * rows))
        return pltpu.make_async_copy(w_sp.at[where], ws.at[where], ws_sem.at[i])

    def mk_copy(i):
        where = (pl.ds(i * rows, rows), pl.ds(0, (i + 1) * rows))
        return pltpu.make_async_copy(mask.at[where], mk.at[where], mk_sem.at[i])

    def own_x():
        return pltpu.make_async_copy(act.at[me], xbuf.at[me], xr_sem.at[me])

    def wo_copy():
        return pltpu.make_async_copy(w_out, wo, wo_sem)

    def x_send(dest):
        return pltpu.make_async_remote_copy(
            src_ref=act.at[dest], dst_ref=xbuf.at[me], send_sem=xs_sem.at[dest], recv_sem=xr_sem.at[me],
            device_id={"seq": dest}, device_id_type=MESH)

    def x_recv(block):
        return pltpu.make_async_remote_copy(
            src_ref=act.at[block], dst_ref=xbuf.at[block], send_sem=xs_sem.at[block], recv_sem=xr_sem.at[block],
            device_id={"seq": block}, device_id_type=MESH)

    def y_send(block):
        return pltpu.make_async_remote_copy(
            src_ref=ybuf.at[block], dst_ref=out.at[me], send_sem=ys_sem.at[block], recv_sem=yr_sem.at[me],
            device_id={"seq": block}, device_id_type=MESH)

    def y_recv(block):
        return pltpu.make_async_remote_copy(
            src_ref=ybuf.at[block], dst_ref=out.at[block], send_sem=ys_sem.at[block], recv_sem=yr_sem.at[block],
            device_id={"seq": block}, device_id_type=MESH)

    def y_own():
        return pltpu.make_async_copy(ybuf.at[me], out.at[me], yr_sem.at[me])

    barrier = pltpu.get_barrier_semaphore()
    for k in range(1, n):
        pl.semaphore_signal(barrier, inc=1, device_id={"seq": lax.rem(me + k, n)}, device_id_type=MESH)
    own_x().start()
    order = list(range(n_cols, 2 * n_cols)) + list(range(n_cols))
    for c in order:
        wi_copy(c).start()
    pl.semaphore_wait(barrier, n - 1)
    for dest in (far, partner, far + 1):
        x_send(dest).start()
    for i in range(n):
        ws_copy(i).start()
        mk_copy(i).start()
    wo_copy().start()

    for i in range(n):
        at = pl.ds(i * rows, rows)
        bias[at, :] = jnp.broadcast_to(b_sp[:, at], (128, rows)).T

    def stage_a(t, first):
        block = lax.rem(2 * chip + t, n)
        at = pl.multiple_of(block * rows, rows)

        @pl.when(block == me)
        def _():
            own_x().wait()

        @pl.when(block != me)
        def _():
            x_recv(block).wait_recv()

        step1 = 64
        for r in range(rows // step1):
            part = pl.ds(r * step1, step1)
            u[part, :] = layer_norm(xbuf[block, part, :].astype(F32), ln1s[...], ln1b[...]).astype(BF16)

        def chunk(c):
            if first:
                wi_copy(c).wait()
            cols = pl.ds(c * COLS, COLS)
            acc = jnp.dot(u[...], wi[:, cols], preferred_element_type=F32)
            return gelu(acc + b_in[:, cols]).astype(BF16)

        for c in range(n_cols):
            vn[pl.ds(at, rows), pl.ds(c * COLS, COLS)] = chunk(n_cols + c)
        for c in range(n_cols):
            g[pl.ds(at, rows), pl.ds(c * COLS, COLS)] = chunk(c)
        step2 = 16

        def norm(r, carry):
            part = pl.ds(pl.multiple_of(at + r * step2, step2), step2)
            vn[part, :] = layer_norm(vn[part, :].astype(F32), ln2s[...], ln2b[...]).astype(BF16)
            return carry

        lax.fori_loop(0, rows // step2, norm, 0)

    def stage_b(i):
        at = pl.ds(i * rows, rows)
        depth = (i + 1) * rows
        ws_copy(i).wait()
        mk_copy(i).wait()
        for r in range(i + 1):
            cols = pl.ds(r * rows, rows)
            ws[at, cols] = jnp.where(mk[at, cols] > 0, ws[at, cols].astype(F32), 0.0).astype(BF16)
        if i == 0:
            wo_copy().wait()
        bias_cols = jnp.concatenate([bias[at, :]] * (COLS // 128), axis=1)
        for c in range(n_cols):
            cols = pl.ds(c * COLS, COLS)
            s = jnp.dot(ws[at, :depth], vn[:depth, cols], preferred_element_type=F32) + bias_cols
            q[:, cols] = (g[at, cols].astype(F32) * s.astype(BF16).astype(F32)).astype(BF16)
        for c in range(width // COLS):
            cols = pl.ds(c * COLS, COLS)
            y = jnp.dot(q[...], wo[:, cols], preferred_element_type=F32) + b_out[:, cols]
            ybuf[i, :, cols] = (xbuf[i, :, cols].astype(F32) + y).astype(BF16)

        @pl.when(me == i)
        def _():
            y_own().start()

        @pl.when(me != i)
        def _():
            y_send(i).start()

    stage_a(0, True)

    def outer(k, carry):
        def upto(k):
            return (1 - chip) * (2 + k // 2 + k // 3) + chip * (3 + (k + 2) // 3)

        def one(t, c):
            stage_a(t, False)
            return c

        low = jnp.where(k == 0, 1, upto(k - 1)) if not isinstance(k, int) else (1 if k == 0 else upto(k - 1))
        lax.fori_loop(low, upto(k), one, 0)
        for i in range(n):
            pl.when(k == i)(functools.partial(stage_b, i))
        return carry

    lax.fori_loop(0, n, outer, 0)

    for k in range(1, n):
        peer = lax.rem(me + k, n)
        x_send(peer).wait_send()
        y_send(peer).wait_send()
        y_recv(peer).wait_recv()
    y_own().wait()


def solution(mesh):
    n = mesh.shape["seq"]
    row_spec = P("data", "seq", None)

    def local_block(act_in, ln1_scale, ln1_bias, w_in, b_in, ln2_scale, ln2_bias, w_spatial, b_spatial, causal_mask, w_out, b_out):
        batch, rows, width = act_in.shape
        length = batch * 0 + n * rows
        gate = w_out.shape[0]
        hbm = pl.BlockSpec(memory_space=pl.ANY)
        vmem = pl.BlockSpec(memory_space=pltpu.VMEM)

        def row(v):
            return v.reshape(1, -1)

        return pl.pallas_call(
            functools.partial(body, n),
            out_shape=jax.ShapeDtypeStruct(act_in.shape, act_in.dtype),
            in_specs=[hbm, vmem, vmem, hbm, vmem, vmem, vmem, hbm, vmem, hbm, hbm, vmem],
            out_specs=hbm,
            scratch_shapes=[
                pltpu.VMEM((n, rows, width), BF16),
                pltpu.VMEM((width, 2 * gate), BF16),
                pltpu.VMEM((gate, width), BF16),
                pltpu.VMEM((length, length), BF16),
                pltpu.VMEM((length, length), jnp.int32),
                pltpu.VMEM((length, gate), BF16),
                pltpu.VMEM((length, gate), BF16),
                pltpu.VMEM((rows, width), BF16),
                pltpu.VMEM((rows, gate), BF16),
                pltpu.VMEM((n, rows, width), BF16),
                pltpu.VMEM((length, 128), F32),
                pltpu.SemaphoreType.DMA((n,)),
                pltpu.SemaphoreType.DMA((n,)),
                pltpu.SemaphoreType.DMA((n,)),
                pltpu.SemaphoreType.DMA((n,)),
                pltpu.SemaphoreType.DMA((2 * gate // COLS,)),
                pltpu.SemaphoreType.DMA,
                pltpu.SemaphoreType.DMA((n,)),
                pltpu.SemaphoreType.DMA((n,)),
            ],
            compiler_params=pltpu.CompilerParams(
                collective_id=0, has_side_effects=True, vmem_limit_bytes=60 * 1024 * 1024),
            name="gmlp",
        )(act_in, row(ln1_scale), row(ln1_bias), w_in, row(b_in), row(ln2_scale), row(ln2_bias),
          w_spatial, row(b_spatial), causal_mask, w_out, row(b_out))

    return jax.shard_map(local_block, mesh=mesh, in_specs=(row_spec,) + (P(),) * 11, out_specs=row_spec, check_vma=False)
```

```python
import functools

import jax
import jax.numpy as jnp
from jax import lax
from jax.experimental import pallas as pl
from jax.experimental.pallas import tpu as pltpu
from jax.sharding import PartitionSpec as P

LN_EPS = 1e-6
GELU_A = 0.7978845608028654
GELU_B = GELU_A * 0.044715
COLS = 512
MESH = pl.DeviceIdType.MESH
F32 = jnp.float32
BF16 = jnp.bfloat16


def gelu(a):
    half = 0.5 * a
    return half + half * jnp.tanh(a * (GELU_A + GELU_B * (a * a)))


def layer_norm(x, gain, shift):
    width = x.shape[-1]
    mean = jnp.sum(x, axis=-1, keepdims=True) * (1.0 / width)
    centered = x - mean
    var = jnp.sum(centered * centered, axis=-1, keepdims=True) * (1.0 / width)
    return centered * lax.rsqrt(var + LN_EPS) * gain + shift


def body(n, act, ln1s, ln1b, w_in, b_in, ln2s, ln2b, w_sp, b_sp, mask, w_out, b_out, out,
         xbuf, wi, wo, ws, mk, h, u, q, ybuf, bias, acc0, acc1,
         xs_sem, xr_sem, ys_sem, yr_sem, wi_sem, wo_sem, ws_sem, mk_sem):
    me = lax.axis_index("seq")
    chip, core = me // 2, lax.rem(me, 2)
    partner = chip * 2 + 1 - core
    far = (1 - chip) * 2
    rows, width = act.shape[1], act.shape[2]
    gate = w_out.shape[0]
    n_cols = gate // COLS

    def cols_of(c):
        return pl.ds(pl.multiple_of(c * COLS, COLS), COLS)

    def rows_of(i):
        return pl.ds(pl.multiple_of(i * rows, rows), rows)

    def wi_copy(c):
        return pltpu.make_async_copy(w_in.at[:, cols_of(c)], wi.at[:, cols_of(c)], wi_sem.at[c])

    def ws_copy(i):
        return pltpu.make_async_copy(w_sp.at[rows_of(i)], ws.at[rows_of(i)], ws_sem.at[i])

    def mk_copy(i):
        return pltpu.make_async_copy(mask.at[rows_of(i)], mk.at[rows_of(i)], mk_sem.at[i])

    def own_x():
        return pltpu.make_async_copy(act.at[me], xbuf.at[me], xr_sem.at[me])

    def wo_copy():
        return pltpu.make_async_copy(w_out, wo, wo_sem)

    def x_send(dest):
        return pltpu.make_async_remote_copy(
            src_ref=act.at[dest], dst_ref=xbuf.at[me], send_sem=xs_sem.at[dest], recv_sem=xr_sem.at[me],
            device_id={"seq": dest}, device_id_type=MESH)

    def x_recv(block):
        return pltpu.make_async_remote_copy(
            src_ref=act.at[block], dst_ref=xbuf.at[block], send_sem=xs_sem.at[block], recv_sem=xr_sem.at[block],
            device_id={"seq": block}, device_id_type=MESH)

    def y_send(block):
        return pltpu.make_async_remote_copy(
            src_ref=ybuf.at[block], dst_ref=out.at[me], send_sem=ys_sem.at[block], recv_sem=yr_sem.at[me],
            device_id={"seq": block}, device_id_type=MESH)

    def y_recv(block):
        return pltpu.make_async_remote_copy(
            src_ref=ybuf.at[block], dst_ref=out.at[block], send_sem=ys_sem.at[block], recv_sem=yr_sem.at[block],
            device_id={"seq": block}, device_id_type=MESH)

    def y_own():
        return pltpu.make_async_copy(ybuf.at[me], out.at[me], yr_sem.at[me])

    barrier = pltpu.get_barrier_semaphore()
    for k in range(1, n):
        pl.semaphore_signal(barrier, inc=1, device_id={"seq": lax.rem(me + k, n)}, device_id_type=MESH)
    own_x().start()
    for c in range(2 * n_cols):
        wi_copy(c).start()
    pl.semaphore_wait(barrier, n - 1)
    for dest in (far, partner, far + 1):
        x_send(dest).start()
    for i in range(n):
        ws_copy(i).start()
        mk_copy(i).start()
    wo_copy().start()

    def stage_a(t):
        block = lax.rem(2 * chip + t, n)
        at = rows_of(block)

        @pl.when(block == me)
        def _():
            own_x().wait()

        @pl.when(block != me)
        def _():
            x_recv(block).wait_recv()

        step1 = 32

        def norm1(r, carry):
            part = pl.ds(pl.multiple_of(r * step1, step1), step1)
            u[part, :] = layer_norm(xbuf[block, part, :].astype(F32), ln1s[...], ln1b[...]).astype(BF16)
            return carry

        lax.fori_loop(0, rows // step1, norm1, 0)

        def dot(c):
            return jnp.dot(u[...], wi[:, cols_of(c)], preferred_element_type=F32)

        def finish(acc, c):
            h[at, cols_of(c)] = gelu(acc[...] + b_in[:, cols_of(c)]).astype(BF16)

        def pair(p, carry):
            c = 2 * p

            @pl.when(t == 0)
            def _():
                wi_copy(c).wait()
                wi_copy(c + 1).wait()

            acc0[...] = dot(c)
            finish(acc1, lax.rem(c + 2 * n_cols - 1, 2 * n_cols))
            acc1[...] = dot(c + 1)
            finish(acc0, c)
            return carry

        lax.fori_loop(0, n_cols, pair, 0)
        finish(acc1, 2 * n_cols - 1)
        step2 = 16

        def norm2(r, carry):
            part = (pl.ds(pl.multiple_of(block * rows + r * step2, step2), step2), pl.ds(gate, gate))
            h[part] = layer_norm(h[part].astype(F32), ln2s[...], ln2b[...]).astype(BF16)
            return carry

        lax.fori_loop(0, rows // step2, norm2, 0)

    def stage_b(i):
        at = rows_of(i)
        bias[...] = jnp.broadcast_to(b_sp[:, at], (128, rows)).T
        ws_copy(i).wait()
        mk_copy(i).wait()
        step = 32

        def select(r, carry):
            part = pl.ds(pl.multiple_of(i * rows + r * step, step), step)
            ws[part, :] = jnp.where(mk[part, :] > 0, ws[part, :].astype(F32), 0.0).astype(BF16)
            return carry

        lax.fori_loop(0, rows // step, select, 0)

        @pl.when(i == 0)
        def _():
            wo_copy().wait()

        def finish(acc, c):
            s = acc[...] + jnp.concatenate([bias[...]] * (COLS // 128), axis=1)
            q[:, cols_of(c)] = (h[at, cols_of(c)].astype(F32) * s.astype(BF16).astype(F32)).astype(BF16)

        def spatial(depth):
            def dot(c):
                return jnp.dot(ws[at, :depth], h[:depth, cols_of(n_cols + c)], preferred_element_type=F32)

            def pair(p, carry):
                c = 2 * p
                acc0[...] = dot(c)
                finish(acc1, lax.rem(c + n_cols - 1, n_cols))
                acc1[...] = dot(c + 1)
                finish(acc0, c)
                return carry

            lax.fori_loop(0, n_cols // 2, pair, 0)

        for k in range(n):
            pl.when(i == k)(functools.partial(spatial, (k + 1) * rows))
        finish(acc1, n_cols - 1)

        def project(c, carry):
            cols = cols_of(c)
            y = jnp.dot(q[...], wo[:, cols], preferred_element_type=F32) + b_out[:, cols]
            ybuf[i, :, cols] = (xbuf[i, :, cols].astype(F32) + y).astype(BF16)
            return carry

        lax.fori_loop(0, width // COLS, project, 0)

        @pl.when(me == i)
        def _():
            y_own().start()

        @pl.when(me != i)
        def _():
            y_send(i).start()

    def outer(k, carry):
        def upto(k):
            return (1 - chip) * (2 + k // 2 + k // 3) + chip * (3 + (k + 2) // 3)

        def one(t, c):
            stage_a(t)
            return c

        lax.fori_loop(jnp.where(k == 0, 0, upto(k - 1)), upto(k), one, 0)
        stage_b(k)
        return carry

    lax.fori_loop(0, n, outer, 0)

    for k in range(1, n):
        peer = lax.rem(me + k, n)
        x_send(peer).wait_send()
        y_send(peer).wait_send()
        y_recv(peer).wait_recv()
    y_own().wait()


def solution(mesh):
    n = mesh.shape["seq"]
    row_spec = P("data", "seq", None)

    def local_block(act_in, ln1_scale, ln1_bias, w_in, b_in, ln2_scale, ln2_bias, w_spatial, b_spatial, causal_mask, w_out, b_out):
        rows, width = act_in.shape[1:]
        length = n * rows
        gate = w_out.shape[0]
        hbm = pl.BlockSpec(memory_space=pl.ANY)
        vmem = pl.BlockSpec(memory_space=pltpu.VMEM)

        def row(v):
            return v.reshape(1, -1)

        return pl.pallas_call(
            functools.partial(body, n),
            out_shape=jax.ShapeDtypeStruct(act_in.shape, act_in.dtype),
            in_specs=[hbm, vmem, vmem, hbm, vmem, vmem, vmem, hbm, vmem, hbm, hbm, vmem],
            out_specs=hbm,
            scratch_shapes=[
                pltpu.VMEM((n, rows, width), BF16),
                pltpu.VMEM((width, 2 * gate), BF16),
                pltpu.VMEM((gate, width), BF16),
                pltpu.VMEM((length, length), BF16),
                pltpu.VMEM((length, length), jnp.int32),
                pltpu.VMEM((length, 2 * gate), BF16),
                pltpu.VMEM((rows, width), BF16),
                pltpu.VMEM((rows, gate), BF16),
                pltpu.VMEM((n, rows, width), BF16),
                pltpu.VMEM((rows, 128), F32),
                pltpu.VMEM((rows, COLS), F32),
                pltpu.VMEM((rows, COLS), F32),
                pltpu.SemaphoreType.DMA((n,)),
                pltpu.SemaphoreType.DMA((n,)),
                pltpu.SemaphoreType.DMA((n,)),
                pltpu.SemaphoreType.DMA((n,)),
                pltpu.SemaphoreType.DMA((2 * gate // COLS,)),
                pltpu.SemaphoreType.DMA,
                pltpu.SemaphoreType.DMA((n,)),
                pltpu.SemaphoreType.DMA((n,)),
            ],
            compiler_params=pltpu.CompilerParams(
                collective_id=0, has_side_effects=True, vmem_limit_bytes=60 * 1024 * 1024),
            name="gmlp",
        )(act_in, row(ln1_scale), row(ln1_bias), w_in, row(b_in), row(ln2_scale), row(ln2_bias),
          w_spatial, row(b_spatial), causal_mask, w_out, row(b_out))

    return jax.shard_map(local_block, mesh=mesh, in_specs=(row_spec,) + (P(),) * 11, out_specs=row_spec, check_vma=False)
```

```python
import functools

import jax
import jax.numpy as jnp
from jax import lax
from jax.experimental import pallas as pl
from jax.experimental.pallas import tpu as pltpu
from jax.sharding import PartitionSpec as P

LN_EPS = 1e-6
GELU_A = 0.7978845608028654
GELU_B = GELU_A * 0.044715
COLS = 512
MESH = pl.DeviceIdType.MESH
F32 = jnp.float32
BF16 = jnp.bfloat16


def gelu(a):
    half = 0.5 * a
    return half + half * jnp.tanh(a * (GELU_A + GELU_B * (a * a)))


def layer_norm(x, gain, shift):
    width = x.shape[-1]
    mean = jnp.sum(x, axis=-1, keepdims=True) * (1.0 / width)
    centered = x - mean
    var = jnp.sum(centered * centered, axis=-1, keepdims=True) * (1.0 / width)
    return centered * lax.rsqrt(var + LN_EPS) * gain + shift


def body(n, act, ln1s, ln1b, w_in, b_in, ln2s, ln2b, w_sp, b_sp, mask, w_out, b_out, out,
         xbuf, wi, wo, ws, mk, vn, g, u, q, ybuf, bias,
         xs_sem, xr_sem, ys_sem, yr_sem, wi_sem, wo_sem, ws_sem, mk_sem):
    me = lax.axis_index("seq")
    chip, core = me // 2, lax.rem(me, 2)
    partner = chip * 2 + 1 - core
    far = (1 - chip) * 2
    rows, width = act.shape[1], act.shape[2]
    gate = w_out.shape[0]
    n_cols = gate // COLS

    def wi_copy(c):
        cols = pl.ds(c * COLS, COLS)
        return pltpu.make_async_copy(w_in.at[:, cols], wi.at[:, cols], wi_sem.at[c])

    def ws_copy(i):
        where = (pl.ds(i * rows, rows), pl.ds(0, (i + 1) * rows))
        return pltpu.make_async_copy(w_sp.at[where], ws.at[where], ws_sem.at[i])

    def mk_copy(i):
        where = (pl.ds(i * rows, rows), pl.ds(0, (i + 1) * rows))
        return pltpu.make_async_copy(mask.at[where], mk.at[where], mk_sem.at[i])

    def own_x():
        return pltpu.make_async_copy(act.at[me], xbuf.at[me], xr_sem.at[me])

    def wo_copy():
        return pltpu.make_async_copy(w_out, wo, wo_sem)

    def x_send(dest):
        return pltpu.make_async_remote_copy(
            src_ref=act.at[dest], dst_ref=xbuf.at[me], send_sem=xs_sem.at[dest], recv_sem=xr_sem.at[me],
            device_id={"seq": dest}, device_id_type=MESH)

    def x_recv(block):
        return pltpu.make_async_remote_copy(
            src_ref=act.at[block], dst_ref=xbuf.at[block], send_sem=xs_sem.at[block], recv_sem=xr_sem.at[block],
            device_id={"seq": block}, device_id_type=MESH)

    def y_send(block):
        return pltpu.make_async_remote_copy(
            src_ref=ybuf.at[block], dst_ref=out.at[me], send_sem=ys_sem.at[block], recv_sem=yr_sem.at[me],
            device_id={"seq": block}, device_id_type=MESH)

    def y_recv(block):
        return pltpu.make_async_remote_copy(
            src_ref=ybuf.at[block], dst_ref=out.at[block], send_sem=ys_sem.at[block], recv_sem=yr_sem.at[block],
            device_id={"seq": block}, device_id_type=MESH)

    def y_own():
        return pltpu.make_async_copy(ybuf.at[me], out.at[me], yr_sem.at[me])

    barrier = pltpu.get_barrier_semaphore()
    for k in range(1, n):
        pl.semaphore_signal(barrier, inc=1, device_id={"seq": lax.rem(me + k, n)}, device_id_type=MESH)
    own_x().start()
    order = list(range(n_cols, 2 * n_cols)) + list(range(n_cols))
    for c in order:
        wi_copy(c).start()
    pl.semaphore_wait(barrier, n - 1)
    for dest in (far, partner, far + 1):
        x_send(dest).start()
    for i in range(n):
        ws_copy(i).start()
        mk_copy(i).start()
    wo_copy().start()

    for i in range(n):
        at = pl.ds(i * rows, rows)
        bias[at, :] = jnp.broadcast_to(b_sp[:, at], (128, rows)).T

    def stage_a(t, first):
        block = lax.rem(2 * chip + t, n)
        at = pl.multiple_of(block * rows, rows)

        @pl.when(block == me)
        def _():
            own_x().wait()

        @pl.when(block != me)
        def _():
            x_recv(block).wait_recv()

        step1 = 64
        for r in range(rows // step1):
            part = pl.ds(r * step1, step1)
            u[part, :] = layer_norm(xbuf[block, part, :].astype(F32), ln1s[...], ln1b[...]).astype(BF16)

        def chunk(c):
            if first:
                wi_copy(c).wait()
            cols = pl.ds(c * COLS, COLS)
            acc = jnp.dot(u[...], wi[:, cols], preferred_element_type=F32)
            return gelu(acc + b_in[:, cols]).astype(BF16)

        step2 = 16
        tiles = rows // step2

        def norm(r):
            part = pl.ds(at + r * step2, step2)
            vn[part, :] = layer_norm(vn[part, :].astype(F32), ln2s[...], ln2b[...]).astype(BF16)

        for c in range(n_cols):
            vn[pl.ds(at, rows), pl.ds(c * COLS, COLS)] = chunk(n_cols + c)
        for c in range(n_cols):
            g[pl.ds(at, rows), pl.ds(c * COLS, COLS)] = chunk(c)
            for r in range(c * tiles // n_cols, (c + 1) * tiles // n_cols):
                norm(r)

    def stage_b(i):
        at = pl.ds(i * rows, rows)
        depth = (i + 1) * rows
        ws_copy(i).wait()
        mk_copy(i).wait()
        for r in range(i + 1):
            cols = pl.ds(r * rows, rows)
            ws[at, cols] = jnp.where(mk[at, cols] > 0, ws[at, cols].astype(F32), 0.0).astype(BF16)
        if i == 0:
            wo_copy().wait()
        bias_cols = jnp.concatenate([bias[at, :]] * (COLS // 128), axis=1)
        for c in range(n_cols):
            cols = pl.ds(c * COLS, COLS)
            s = jnp.dot(ws[at, :depth], vn[:depth, cols], preferred_element_type=F32) + bias_cols
            q[:, cols] = (g[at, cols].astype(F32) * s.astype(BF16).astype(F32)).astype(BF16)
        for c in range(width // COLS):
            cols = pl.ds(c * COLS, COLS)
            y = jnp.dot(q[...], wo[:, cols], preferred_element_type=F32) + b_out[:, cols]
            ybuf[i, :, cols] = (xbuf[i, :, cols].astype(F32) + y).astype(BF16)

        @pl.when(me == i)
        def _():
            y_own().start()

        @pl.when(me != i)
        def _():
            y_send(i).start()

    stage_a(0, True)

    def outer(k, carry):
        def upto(k):
            return (1 - chip) * (2 + k // 2 + k // 3) + chip * (3 + (k + 2) // 3)

        def one(t, c):
            stage_a(t, False)
            return c

        low = jnp.where(k == 0, 1, upto(k - 1)) if not isinstance(k, int) else (1 if k == 0 else upto(k - 1))
        lax.fori_loop(low, upto(k), one, 0)
        for i in range(n):
            pl.when(k == i)(functools.partial(stage_b, i))
        return carry

    lax.fori_loop(0, n, outer, 0)

    for k in range(1, n):
        peer = lax.rem(me + k, n)
        x_send(peer).wait_send()
        y_send(peer).wait_send()
        y_recv(peer).wait_recv()
    y_own().wait()


def solution(mesh):
    n = mesh.shape["seq"]
    row_spec = P("data", "seq", None)

    def local_block(act_in, ln1_scale, ln1_bias, w_in, b_in, ln2_scale, ln2_bias, w_spatial, b_spatial, causal_mask, w_out, b_out):
        rows, width = act_in.shape[1:]
        length = n * rows
        gate = w_out.shape[0]
        hbm = pl.BlockSpec(memory_space=pl.ANY)
        vmem = pl.BlockSpec(memory_space=pltpu.VMEM)

        def row(v):
            return v.reshape(1, -1)

        return pl.pallas_call(
            functools.partial(body, n),
            out_shape=jax.ShapeDtypeStruct(act_in.shape, act_in.dtype),
            in_specs=[hbm, vmem, vmem, hbm, vmem, vmem, vmem, hbm, vmem, hbm, hbm, vmem],
            out_specs=hbm,
            scratch_shapes=[
                pltpu.VMEM((n, rows, width), BF16),
                pltpu.VMEM((width, 2 * gate), BF16),
                pltpu.VMEM((gate, width), BF16),
                pltpu.VMEM((length, length), BF16),
                pltpu.VMEM((length, length), jnp.int32),
                pltpu.VMEM((length, gate), BF16),
                pltpu.VMEM((length, gate), BF16),
                pltpu.VMEM((rows, width), BF16),
                pltpu.VMEM((rows, gate), BF16),
                pltpu.VMEM((n, rows, width), BF16),
                pltpu.VMEM((length, 128), F32),
                pltpu.SemaphoreType.DMA((n,)),
                pltpu.SemaphoreType.DMA((n,)),
                pltpu.SemaphoreType.DMA((n,)),
                pltpu.SemaphoreType.DMA((n,)),
                pltpu.SemaphoreType.DMA((2 * gate // COLS,)),
                pltpu.SemaphoreType.DMA,
                pltpu.SemaphoreType.DMA((n,)),
                pltpu.SemaphoreType.DMA((n,)),
            ],
            compiler_params=pltpu.CompilerParams(
                collective_id=0, has_side_effects=True, vmem_limit_bytes=60 * 1024 * 1024),
            name="gmlp",
        )(act_in, row(ln1_scale), row(ln1_bias), w_in, row(b_in), row(ln2_scale), row(ln2_bias),
          w_spatial, row(b_spatial), causal_mask, w_out, row(b_out))

    return jax.shard_map(local_block, mesh=mesh, in_specs=(row_spec,) + (P(),) * 11, out_specs=row_spec, check_vma=False)
```

```python
import functools

import jax
import jax.numpy as jnp
from jax import lax
from jax.experimental import pallas as pl
from jax.experimental.pallas import tpu as pltpu
from jax.sharding import PartitionSpec as P

LN_EPS = 1e-6
GELU_A = 0.7978845608028654
GELU_B = GELU_A * 0.044715
COLS = 512
MESH = pl.DeviceIdType.MESH
F32 = jnp.float32
BF16 = jnp.bfloat16


def gelu(a):
    return a * jax.nn.sigmoid(a * (2 * GELU_A + 2 * GELU_B * (a * a)))


def layer_norm(x, gain, shift):
    width = x.shape[-1]
    mean = jnp.sum(x, axis=-1, keepdims=True) * (1.0 / width)
    centered = x - mean
    var = jnp.sum(centered * centered, axis=-1, keepdims=True) * (1.0 / width)
    return centered * lax.rsqrt(var + LN_EPS) * gain + shift


def body(n, act, ln1s, ln1b, w_in, b_in, ln2s, ln2b, w_sp, b_sp, mask, w_out, b_out, out,
         xbuf, wi, wo, ws, mk, vn, g, u, q, ybuf, bias, stat,
         xs_sem, xr_sem, ys_sem, yr_sem, wi_sem, wo_sem, ws_sem, mk_sem):
    me = lax.axis_index("seq")
    chip, core = me // 2, lax.rem(me, 2)
    partner = chip * 2 + 1 - core
    far = (1 - chip) * 2
    rows, width = act.shape[1], act.shape[2]
    half = rows // 2
    gate = w_out.shape[0]
    n_cols = gate // COLS

    def wi_copy(c):
        cols = pl.ds(c * COLS, COLS)
        return pltpu.make_async_copy(w_in.at[:, cols], wi.at[:, cols], wi_sem.at[c])

    def ws_copy(i):
        where = (pl.ds(i * rows, rows), pl.ds(0, (i + 1) * rows))
        return pltpu.make_async_copy(w_sp.at[where], ws.at[where], ws_sem.at[i])

    def mk_copy(i):
        where = (pl.ds(i * rows, rows), pl.ds(0, (i + 1) * rows))
        return pltpu.make_async_copy(mask.at[where], mk.at[where], mk_sem.at[i])

    def wo_copy():
        return pltpu.make_async_copy(w_out, wo, wo_sem)

    def own_x(p):
        part = pl.ds(p * half, half)
        return pltpu.make_async_copy(act.at[me, part], xbuf.at[me, part], xr_sem.at[me, p])

    def x_send(dest, p):
        part = pl.ds(p * half, half)
        return pltpu.make_async_remote_copy(
            src_ref=act.at[dest, part], dst_ref=xbuf.at[me, part], send_sem=xs_sem.at[dest, p], recv_sem=xr_sem.at[me, p],
            device_id={"seq": dest}, device_id_type=MESH)

    def x_recv(block, p):
        part = pl.ds(p * half, half)
        return pltpu.make_async_remote_copy(
            src_ref=act.at[block, part], dst_ref=xbuf.at[block, part], send_sem=xs_sem.at[block, p],
            recv_sem=xr_sem.at[block, p], device_id={"seq": block}, device_id_type=MESH)

    def y_send(block, c):
        cols = pl.ds(c * COLS, COLS)
        return pltpu.make_async_remote_copy(
            src_ref=ybuf.at[block, :, cols], dst_ref=out.at[me, :, cols], send_sem=ys_sem.at[block, c],
            recv_sem=yr_sem.at[me, c], device_id={"seq": block}, device_id_type=MESH)

    def y_recv(block, c):
        cols = pl.ds(c * COLS, COLS)
        return pltpu.make_async_remote_copy(
            src_ref=ybuf.at[block, :, cols], dst_ref=out.at[block, :, cols], send_sem=ys_sem.at[block, c],
            recv_sem=yr_sem.at[block, c], device_id={"seq": block}, device_id_type=MESH)

    def y_own(c):
        cols = pl.ds(c * COLS, COLS)
        return pltpu.make_async_copy(ybuf.at[me, :, cols], out.at[me, :, cols], yr_sem.at[me, c])

    barrier = pltpu.get_barrier_semaphore()
    for k in range(1, n):
        pl.semaphore_signal(barrier, inc=1, device_id={"seq": lax.rem(me + k, n)}, device_id_type=MESH)
    for p in range(2):
        own_x(p).start()
    order = list(range(n_cols, 2 * n_cols)) + list(range(n_cols))
    for c in order:
        wi_copy(c).start()
    pl.semaphore_wait(barrier, n - 1)
    for dest in (far, partner, far + 1):
        for p in range(2):
            x_send(dest, p).start()
    for i in range(n):
        ws_copy(i).start()
        mk_copy(i).start()
    wo_copy().start()

    for i in range(n):
        at = pl.ds(i * rows, rows)
        bias[at, :] = jnp.broadcast_to(b_sp[:, at], (128, rows)).T

    def stage_a(t, first):
        if first:
            pieces = [(me, 0), (me, 1)]
            for p in range(2):
                own_x(p).wait()
        else:
            remote = t // 2
            side = t - 2
            pieces = [((1 - remote) * partner + remote * far, remote * side),
                      ((1 - remote) * partner + remote * (far + 1), (1 - remote) + remote * side)]
            for block, p in pieces:
                x_recv(block, p).wait_recv()
        starts = [pl.multiple_of(block * rows + p * half, half) for block, p in pieces]
        step1 = 64
        for k, (block, p) in enumerate(pieces):
            for r in range(half // step1):
                x = xbuf[block, pl.ds(pl.multiple_of(p * half, half) + r * step1, step1), :].astype(F32)
                u[pl.ds(k * half + r * step1, step1), :] = layer_norm(x, ln1s[...], ln1b[...]).astype(BF16)

        def chunk(c, dst, dst_c):
            if first:
                wi_copy(c).wait()
            cols = pl.ds(c * COLS, COLS)
            acc = jnp.dot(u[...], wi[:, cols], preferred_element_type=F32)
            value = gelu(acc + b_in[:, cols]).astype(BF16)
            for k in range(2):
                dst[pl.ds(starts[k], half), pl.ds(dst_c * COLS, COLS)] = value[k * half:(k + 1) * half]
            return value

        lanes = 128
        per_lane = gate // lanes
        for c in range(n_cols):
            value = chunk(n_cols + c, vn, c).astype(F32)
            tiles = [value[:, j * lanes:(j + 1) * lanes] for j in range(COLS // lanes)]
            if c == 0:
                pivot = tiles[0]
                stat[0] = pivot
                tiles = tiles[1:]
            else:
                pivot = stat[0]
            diffs = [v - pivot for v in tiles]
            total = sum(diffs[1:], diffs[0])
            squares = sum([d * d for d in diffs[1:]], diffs[0] * diffs[0])
            stat[1] = total if c == 0 else stat[1] + total
            stat[2] = squares if c == 0 else stat[2] + squares
        total = stat[1]
        mean_lane = stat[0] + total * (1.0 / per_lane)
        mean = jnp.sum(mean_lane, axis=-1, keepdims=True) * (1.0 / lanes)
        away = mean_lane - mean
        spread = (stat[2] - total * total * (1.0 / per_lane)) + per_lane * (away * away)
        var = jnp.maximum(jnp.sum(spread, axis=-1, keepdims=True) * (1.0 / gate), 0.0)
        stat[0] = jnp.broadcast_to(mean, (rows, lanes))
        stat[1] = jnp.broadcast_to(lax.rsqrt(var + LN_EPS), (rows, lanes))
        step2 = 16
        tiles = rows // step2

        def norm(r):
            part = pl.ds(starts[r * step2 // half] + r * step2 % half, step2)
            here = pl.ds(r * step2, step2)
            mean = jnp.concatenate([stat[0, here]] * per_lane, axis=1)
            scale = jnp.concatenate([stat[1, here]] * per_lane, axis=1)
            vn[part, :] = ((vn[part, :].astype(F32) - mean) * scale * ln2s[...] + ln2b[...]).astype(BF16)

        for c in range(n_cols):
            chunk(c, g, c)
            for r in range(c * tiles // n_cols, (c + 1) * tiles // n_cols):
                norm(r)

    def stage_b(i):
        at = pl.ds(i * rows, rows)
        depth = (i + 1) * rows
        ws_copy(i).wait()
        mk_copy(i).wait()
        for r in range(i + 1):
            cols = pl.ds(r * rows, rows)
            ws[at, cols] = jnp.where(mk[at, cols] > 0, ws[at, cols].astype(F32), 0.0).astype(BF16)
        bias_cols = jnp.concatenate([bias[at, :]] * (COLS // 128), axis=1)
        for c in range(n_cols):
            cols = pl.ds(c * COLS, COLS)
            s = jnp.dot(ws[at, :depth], vn[:depth, cols], preferred_element_type=F32) + bias_cols
            q[:, cols] = (g[at, cols].astype(F32) * s.astype(BF16).astype(F32)).astype(BF16)
        for c in range(width // COLS):
            cols = pl.ds(c * COLS, COLS)
            y = jnp.dot(q[...], wo[:, cols], preferred_element_type=F32) + b_out[:, cols]
            ybuf[i, :, cols] = (xbuf[i, :, cols].astype(F32) + y).astype(BF16)

            @pl.when(me == i)
            def _():
                y_own(c).start()

            @pl.when(me != i)
            def _():
                y_send(i, c).start()

    stage_a(0, True)
    even0 = (1 - chip) * (1 - core)
    odd0 = (1 - chip) * core

    def outer(k, carry):
        def upto(k):
            return n - 2 * odd0 * (1 - k // 2)

        def one(t, c):
            stage_a(t, False)
            return c

        lax.fori_loop(jnp.where(k == 0, 1, upto(k - 1)), upto(k), one, 0)

        @pl.when(k == 0)
        def _():
            wo_copy().wait()

        block = lax.rem(k + 2 * even0, n)
        for i in range(n):
            pl.when(block == i)(functools.partial(stage_b, i))
        return carry

    lax.fori_loop(0, n, outer, 0)

    for k in range(1, n):
        peer = lax.rem(me + k, n)
        for p in range(2):
            x_send(peer, p).wait_send()
            y_send(peer, p).wait_send()
            y_recv(peer, p).wait_recv()
    for p in range(2):
        y_own(p).wait()


def solution(mesh):
    n = mesh.shape["seq"]
    row_spec = P("data", "seq", None)

    def local_block(act_in, ln1_scale, ln1_bias, w_in, b_in, ln2_scale, ln2_bias, w_spatial, b_spatial, causal_mask, w_out, b_out):
        rows, width = act_in.shape[1:]
        length = n * rows
        gate = w_out.shape[0]
        hbm = pl.BlockSpec(memory_space=pl.ANY)
        vmem = pl.BlockSpec(memory_space=pltpu.VMEM)

        def row(v):
            return v.reshape(1, -1)

        return pl.pallas_call(
            functools.partial(body, n),
            out_shape=jax.ShapeDtypeStruct(act_in.shape, act_in.dtype),
            in_specs=[hbm, vmem, vmem, hbm, vmem, vmem, vmem, hbm, vmem, hbm, hbm, vmem],
            out_specs=hbm,
            scratch_shapes=[
                pltpu.VMEM((n, rows, width), BF16),
                pltpu.VMEM((width, 2 * gate), BF16),
                pltpu.VMEM((gate, width), BF16),
                pltpu.VMEM((length, length), BF16),
                pltpu.VMEM((length, length), jnp.int32),
                pltpu.VMEM((length, gate), BF16),
                pltpu.VMEM((length, gate), BF16),
                pltpu.VMEM((rows, width), BF16),
                pltpu.VMEM((rows, gate), BF16),
                pltpu.VMEM((n, rows, width), BF16),
                pltpu.VMEM((length, 128), F32),
                pltpu.VMEM((3, rows, 128), F32),
                pltpu.SemaphoreType.DMA((n, 2)),
                pltpu.SemaphoreType.DMA((n, 2)),
                pltpu.SemaphoreType.DMA((n, width // COLS)),
                pltpu.SemaphoreType.DMA((n, width // COLS)),
                pltpu.SemaphoreType.DMA((2 * gate // COLS,)),
                pltpu.SemaphoreType.DMA,
                pltpu.SemaphoreType.DMA((n,)),
                pltpu.SemaphoreType.DMA((n,)),
            ],
            compiler_params=pltpu.CompilerParams(
                collective_id=0, has_side_effects=True, vmem_limit_bytes=60 * 1024 * 1024),
            name="gmlp",
        )(act_in, row(ln1_scale), row(ln1_bias), w_in, row(b_in), row(ln2_scale), row(ln2_bias),
          w_spatial, row(b_spatial), causal_mask, w_out, row(b_out))

    return jax.shard_map(local_block, mesh=mesh, in_specs=(row_spec,) + (P(),) * 11, out_specs=row_spec, check_vma=False)
```

```python
import functools

import jax
import jax.numpy as jnp
from jax import lax
from jax.experimental import pallas as pl
from jax.experimental.pallas import tpu as pltpu
from jax.sharding import PartitionSpec as P

LN_EPS = 1e-6
GELU_A = 0.7978845608028654
GELU_B = GELU_A * 0.044715
COLS = 512
LANES = 128
MESH = pl.DeviceIdType.MESH
F32 = jnp.float32
BF16 = jnp.bfloat16


def gelu(a):
    return a * jax.nn.sigmoid(a * (2 * GELU_A + 2 * GELU_B * (a * a)))


def layer_norm(x, gain, shift):
    width = x.shape[-1]
    mean = jnp.sum(x, axis=-1, keepdims=True) * (1.0 / width)
    centered = x - mean
    var = jnp.sum(centered * centered, axis=-1, keepdims=True) * (1.0 / width)
    return centered * lax.rsqrt(var + LN_EPS) * gain + shift


def wide(ref, tiles, *where):
    return jnp.concatenate([ref[(j, *where)] for j in tiles], axis=1)


def body(n, act, ln1s, ln1b, w_in, b_in, ln2s, ln2b, w_sp, b_sp, mask, w_out, b_out, out,
         xbuf, wi, wo, ws, mk, vn, g, u, q, ybuf, bias, stat,
         xs_sem, xr_sem, ys_sem, yr_sem, wi_sem, wo_sem, ws_sem, mk_sem):
    me = lax.axis_index("seq")
    chip, core = me // 2, lax.rem(me, 2)
    partner = chip * 2 + 1 - core
    far = (1 - chip) * 2
    rows, width = act.shape[1], act.shape[2]
    length = n * rows
    half = rows // 2
    gate = w_out.shape[0]
    gate_tiles = gate // LANES
    n_cols = gate // COLS
    per = COLS // LANES

    def lanes(j):
        return pl.ds(j * LANES, LANES)

    def wi_copy(j):
        return pltpu.make_async_copy(w_in.at[:, lanes(j)], wi.at[j], wi_sem.at[j])

    def ws_copy(j):
        return pltpu.make_async_copy(w_sp.at[:, lanes(j)], ws.at[j], ws_sem.at[j])

    def wo_copy(j):
        return pltpu.make_async_copy(w_out.at[:, lanes(j)], wo.at[j], wo_sem.at[j])

    def mk_copy():
        return pltpu.make_async_copy(mask, mk, mk_sem)

    def own_x(p):
        part = pl.ds(p * half, half)
        return pltpu.make_async_copy(act.at[me, part], xbuf.at[me, part], xr_sem.at[me, p])

    def x_send(dest, p):
        part = pl.ds(p * half, half)
        return pltpu.make_async_remote_copy(
            src_ref=act.at[dest, part], dst_ref=xbuf.at[me, part], send_sem=xs_sem.at[dest, p], recv_sem=xr_sem.at[me, p],
            device_id={"seq": dest}, device_id_type=MESH)

    def x_recv(block, p):
        part = pl.ds(p * half, half)
        return pltpu.make_async_remote_copy(
            src_ref=act.at[block, part], dst_ref=xbuf.at[block, part], send_sem=xs_sem.at[block, p],
            recv_sem=xr_sem.at[block, p], device_id={"seq": block}, device_id_type=MESH)

    def y_send(block):
        return pltpu.make_async_remote_copy(
            src_ref=ybuf.at[block], dst_ref=out.at[me], send_sem=ys_sem.at[block], recv_sem=yr_sem.at[me],
            device_id={"seq": block}, device_id_type=MESH)

    def y_recv(block):
        return pltpu.make_async_remote_copy(
            src_ref=ybuf.at[block], dst_ref=out.at[block], send_sem=ys_sem.at[block], recv_sem=yr_sem.at[block],
            device_id={"seq": block}, device_id_type=MESH)

    def y_own():
        return pltpu.make_async_copy(ybuf.at[me], out.at[me], yr_sem.at[me])

    barrier = pltpu.get_barrier_semaphore()
    for k in range(1, n):
        pl.semaphore_signal(barrier, inc=1, device_id={"seq": lax.rem(me + k, n)}, device_id_type=MESH)
    for p in range(2):
        own_x(p).start()
    for j in range(2 * gate_tiles):
        wi_copy((j + gate_tiles) % (2 * gate_tiles)).start()
    pl.semaphore_wait(barrier, n - 1)
    for dest in (far, partner, far + 1):
        for p in range(2):
            x_send(dest, p).start()
    for j in range(length // LANES):
        ws_copy(j).start()
    mk_copy().start()
    for j in range(width // LANES):
        wo_copy(j).start()

    for i in range(n):
        at = pl.ds(i * rows, rows)
        bias[at, :] = jnp.broadcast_to(b_sp[:, at], (LANES, rows)).T

    def stage_a(t, first):
        if first:
            pieces = [(me, 0), (me, 1)]
            for p in range(2):
                own_x(p).wait()
        else:
            remote = t // 2
            side = t - 2
            pieces = [((1 - remote) * partner + remote * far, remote * side),
                      ((1 - remote) * partner + remote * (far + 1), (1 - remote) + remote * side)]
            for block, p in pieces:
                x_recv(block, p).wait_recv()
        starts = [pl.multiple_of(block * rows + p * half, half) for block, p in pieces]
        step1 = 64
        for k, (block, p) in enumerate(pieces):
            for r in range(half // step1):
                x = xbuf[block, pl.ds(pl.multiple_of(p * half, half) + r * step1, step1), :].astype(F32)
                x = layer_norm(x, ln1s[...], ln1b[...]).astype(BF16)
                for j in range(width // LANES):
                    u[j, pl.ds(k * half + r * step1, step1), :] = x[:, j * LANES:(j + 1) * LANES]

        def chunk(c):
            tiles = range(c * per, (c + 1) * per)
            acc = jnp.dot(wide(u, range(width // LANES)), wide(wi, tiles), preferred_element_type=F32)
            return gelu(acc + b_in[:, pl.ds(c * COLS, COLS)]).astype(BF16)

        def put(dst, c, value):
            for j in range(per):
                for k in range(2):
                    dst[c * per + j, pl.ds(starts[k], half), :] = value[k * half:(k + 1) * half, j * LANES:(j + 1) * LANES]

        if first:
            for j in range(gate_tiles, 2 * gate_tiles):
                wi_copy(j).wait()
        for c in range(n_cols):
            value = chunk(n_cols + c)
            put(vn, c, value)
            value = value.astype(F32)
            tiles = [value[:, j * LANES:(j + 1) * LANES] for j in range(per)]
            if c == 0:
                pivot = tiles[0]
                stat[0] = pivot
                tiles = tiles[1:]
            else:
                pivot = stat[0]
            diffs = [v - pivot for v in tiles]
            total = sum(diffs[1:], diffs[0])
            squares = sum([d * d for d in diffs[1:]], diffs[0] * diffs[0])
            stat[1] = total if c == 0 else stat[1] + total
            stat[2] = squares if c == 0 else stat[2] + squares
        if first:
            for j in range(gate_tiles):
                wi_copy(j).wait()
        total = stat[1]
        mean_lane = stat[0] + total * (1.0 / gate_tiles)
        mean = jnp.sum(mean_lane, axis=-1, keepdims=True) * (1.0 / LANES)
        away = mean_lane - mean
        spread = (stat[2] - total * total * (1.0 / gate_tiles)) + gate_tiles * (away * away)
        var = jnp.maximum(jnp.sum(spread, axis=-1, keepdims=True) * (1.0 / gate), 0.0)
        stat[0] = jnp.broadcast_to(mean, (rows, LANES))
        stat[1] = jnp.broadcast_to(lax.rsqrt(var + LN_EPS), (rows, LANES))

        def norm(j):
            for k in range(2):
                part = pl.ds(starts[k], half)
                here = pl.ds(k * half, half)
                value = (vn[j, part, :].astype(F32) - stat[0, here]) * stat[1, here]
                vn[j, part, :] = (value * ln2s[:, lanes(j)] + ln2b[:, lanes(j)]).astype(BF16)

        for c in range(n_cols):
            put(g, c, chunk(c))
            for j in range(c * per, (c + 1) * per):
                norm(j)

    def stage_b(i):
        at = pl.ds(i * rows, rows)
        depth = (i + 1) * rows
        for j in range(depth // LANES):
            ws[j, at, :] = jnp.where(mk[at, lanes(j)] > 0, ws[j, at, :].astype(F32), 0.0).astype(BF16)
        for c in range(n_cols):
            tiles = range(c * per, (c + 1) * per)
            s = jnp.dot(wide(ws, range(depth // LANES), at), wide(vn, tiles, pl.ds(0, depth)), preferred_element_type=F32)
            for j in range(per):
                t = (s[:, j * LANES:(j + 1) * LANES] + bias[at, :]).astype(BF16).astype(F32)
                q[tiles[j]] = (g[tiles[j], at, :].astype(F32) * t).astype(BF16)
        for c in range(width // COLS):
            cols = pl.ds(c * COLS, COLS)
            y = jnp.dot(wide(q, range(gate_tiles)), wide(wo, range(c * per, (c + 1) * per)), preferred_element_type=F32)
            ybuf[i, :, cols] = (xbuf[i, :, cols].astype(F32) + (y + b_out[:, cols])).astype(BF16)

    stage_a(0, True)
    even0 = (1 - chip) * (1 - core)
    odd0 = (1 - chip) * core

    def outer(k, carry):
        def upto(k):
            return n - 2 * odd0 * (1 - k // 2)

        def one(t, c):
            stage_a(t, False)
            return c

        lax.fori_loop(jnp.where(k == 0, 1, upto(k - 1)), upto(k), one, 0)

        @pl.when(k == 0)
        def _():
            for j in range(length // LANES):
                ws_copy(j).wait()
            mk_copy().wait()
            for j in range(width // LANES):
                wo_copy(j).wait()

        block = lax.rem(k + 2 * even0, n)
        for i in range(n):
            pl.when(block == i)(functools.partial(stage_b, i))

        @pl.when(me == block)
        def _():
            y_own().start()

        @pl.when(me != block)
        def _():
            y_send(block).start()

        return carry

    lax.fori_loop(0, n, outer, 0)

    for k in range(1, n):
        peer = lax.rem(me + k, n)
        for p in range(2):
            x_send(peer, p).wait_send()
        y_send(peer).wait_send()
        y_recv(peer).wait_recv()
    y_own().wait()


def solution(mesh):
    n = mesh.shape["seq"]
    row_spec = P("data", "seq", None)

    def local_block(act_in, ln1_scale, ln1_bias, w_in, b_in, ln2_scale, ln2_bias, w_spatial, b_spatial, causal_mask, w_out, b_out):
        rows, width = act_in.shape[1:]
        length = n * rows
        gate = w_out.shape[0]
        hbm = pl.BlockSpec(memory_space=pl.ANY)
        vmem = pl.BlockSpec(memory_space=pltpu.VMEM)

        def row(v):
            return v.reshape(1, -1)

        return pl.pallas_call(
            functools.partial(body, n),
            out_shape=jax.ShapeDtypeStruct(act_in.shape, act_in.dtype),
            in_specs=[hbm, vmem, vmem, hbm, vmem, vmem, vmem, hbm, vmem, hbm, hbm, vmem],
            out_specs=hbm,
            scratch_shapes=[
                pltpu.VMEM((n, rows, width), BF16),
                pltpu.VMEM((2 * gate // LANES, width, LANES), BF16),
                pltpu.VMEM((width // LANES, gate, LANES), BF16),
                pltpu.VMEM((length // LANES, length, LANES), BF16),
                pltpu.VMEM((length, length), jnp.int32),
                pltpu.VMEM((gate // LANES, length, LANES), BF16),
                pltpu.VMEM((gate // LANES, length, LANES), BF16),
                pltpu.VMEM((width // LANES, rows, LANES), BF16),
                pltpu.VMEM((gate // LANES, rows, LANES), BF16),
                pltpu.VMEM((n, rows, width), BF16),
                pltpu.VMEM((length, LANES), F32),
                pltpu.VMEM((3, rows, LANES), F32),
                pltpu.SemaphoreType.DMA((n, 2)),
                pltpu.SemaphoreType.DMA((n, 2)),
                pltpu.SemaphoreType.DMA((n,)),
                pltpu.SemaphoreType.DMA((n,)),
                pltpu.SemaphoreType.DMA((2 * gate // LANES,)),
                pltpu.SemaphoreType.DMA((width // LANES,)),
                pltpu.SemaphoreType.DMA((length // LANES,)),
                pltpu.SemaphoreType.DMA,
            ],
            compiler_params=pltpu.CompilerParams(
                collective_id=0, has_side_effects=True, vmem_limit_bytes=60 * 1024 * 1024),
            name="gmlp",
        )(act_in, row(ln1_scale), row(ln1_bias), w_in, row(b_in), row(ln2_scale), row(ln2_bias),
          w_spatial, row(b_spatial), causal_mask, w_out, row(b_out))

    return jax.shard_map(local_block, mesh=mesh, in_specs=(row_spec,) + (P(),) * 11, out_specs=row_spec, check_vma=False)
```

```python
import functools

import jax
import jax.numpy as jnp
from jax import lax
from jax.experimental import pallas as pl
from jax.experimental.pallas import tpu as pltpu
from jax.sharding import PartitionSpec as P

LN_EPS = 1e-6
GELU_A = 0.7978845608028654
GELU_B = GELU_A * 0.044715
COLS = 512
LANES = 128
MESH = pl.DeviceIdType.MESH
F32 = jnp.float32
BF16 = jnp.bfloat16


def gelu(a):
    return a * jax.nn.sigmoid(a * (2 * GELU_A + 2 * GELU_B * (a * a)))


def layer_norm(x, gain, shift):
    width = x.shape[-1]
    mean = jnp.sum(x, axis=-1, keepdims=True) * (1.0 / width)
    centered = x - mean
    var = jnp.sum(centered * centered, axis=-1, keepdims=True) * (1.0 / width)
    return centered * lax.rsqrt(var + LN_EPS) * gain + shift


def wide(ref, tiles, *where):
    return jnp.concatenate([ref[(j, *where)] for j in tiles], axis=1)


def body(n, act, ln1s, ln1b, w_in, b_in, ln2s, ln2b, w_sp, b_sp, mask, w_out, b_out, out,
         xbuf, wi, wo, ws, mk, vn, g, u, q, ybuf, bias, stat,
         xs_sem, xr_sem, ys_sem, yr_sem, wi_sem, wo_sem, ws_sem, mk_sem):
    me = lax.axis_index("seq")
    chip, core = me // 2, lax.rem(me, 2)
    partner = chip * 2 + 1 - core
    far = (1 - chip) * 2
    rows, width = act.shape[1], act.shape[2]
    length = n * rows
    half = rows // 2
    gate = w_out.shape[0]
    gate_tiles = gate // LANES
    n_cols = gate // COLS
    per = COLS // LANES

    def lanes(j):
        return pl.ds(j * LANES, LANES)

    def wi_copy(j):
        return pltpu.make_async_copy(w_in.at[:, lanes(j)], wi.at[j], wi_sem.at[j])

    def ws_copy(j):
        return pltpu.make_async_copy(w_sp.at[:, lanes(j)], ws.at[j], ws_sem.at[j])

    def wo_copy(j):
        return pltpu.make_async_copy(w_out.at[:, lanes(j)], wo.at[j], wo_sem.at[j])

    def mk_copy():
        return pltpu.make_async_copy(mask, mk, mk_sem)

    def own_x(p):
        part = pl.ds(p * half, half)
        return pltpu.make_async_copy(act.at[me, part], xbuf.at[me, part], xr_sem.at[me, p])

    def x_send(dest, p):
        part = pl.ds(p * half, half)
        return pltpu.make_async_remote_copy(
            src_ref=act.at[dest, part], dst_ref=xbuf.at[me, part], send_sem=xs_sem.at[dest, p], recv_sem=xr_sem.at[me, p],
            device_id={"seq": dest}, device_id_type=MESH)

    def x_recv(block, p):
        part = pl.ds(p * half, half)
        return pltpu.make_async_remote_copy(
            src_ref=act.at[block, part], dst_ref=xbuf.at[block, part], send_sem=xs_sem.at[block, p],
            recv_sem=xr_sem.at[block, p], device_id={"seq": block}, device_id_type=MESH)

    def y_send(block):
        return pltpu.make_async_remote_copy(
            src_ref=ybuf.at[block], dst_ref=out.at[me], send_sem=ys_sem.at[block], recv_sem=yr_sem.at[me],
            device_id={"seq": block}, device_id_type=MESH)

    def y_recv(block):
        return pltpu.make_async_remote_copy(
            src_ref=ybuf.at[block], dst_ref=out.at[block], send_sem=ys_sem.at[block], recv_sem=yr_sem.at[block],
            device_id={"seq": block}, device_id_type=MESH)

    def y_own():
        return pltpu.make_async_copy(ybuf.at[me], out.at[me], yr_sem.at[me])

    barrier = pltpu.get_barrier_semaphore()
    for k in range(1, n):
        pl.semaphore_signal(barrier, inc=1, device_id={"seq": lax.rem(me + k, n)}, device_id_type=MESH)
    for p in range(2):
        own_x(p).start()
    for j in range(2 * gate_tiles):
        wi_copy((j + gate_tiles) % (2 * gate_tiles)).start()
    pl.semaphore_wait(barrier, n - 1)
    for dest in (far, partner, far + 1):
        for p in range(2):
            x_send(dest, p).start()
    for j in range(length // LANES):
        ws_copy(j).start()
    mk_copy().start()
    for j in range(width // LANES):
        wo_copy(j).start()

    for i in range(n):
        at = pl.ds(i * rows, rows)
        bias[at, :] = jnp.broadcast_to(b_sp[:, at], (LANES, rows)).T

    def stage_a(t, first):
        if first:
            pieces = [(me, 0), (me, 1)]
            for p in range(2):
                own_x(p).wait()
        else:
            remote = t // 2
            side = t - 2
            pieces = [((1 - remote) * partner + remote * far, remote * side),
                      ((1 - remote) * partner + remote * (far + 1), (1 - remote) + remote * side)]
            for block, p in pieces:
                x_recv(block, p).wait_recv()
        starts = [pl.multiple_of(block * rows + p * half, half) for block, p in pieces]
        step1 = 64
        for k, (block, p) in enumerate(pieces):
            for r in range(half // step1):
                x = xbuf[block, pl.ds(pl.multiple_of(p * half, half) + r * step1, step1), :].astype(F32)
                x = layer_norm(x, ln1s[...], ln1b[...]).astype(BF16)
                for j in range(width // LANES):
                    u[j, pl.ds(k * half + r * step1, step1), :] = x[:, j * LANES:(j + 1) * LANES]

        def chunk(c):
            tiles = range(c * per, (c + 1) * per)
            acc = jnp.dot(wide(u, range(width // LANES)), wide(wi, tiles), preferred_element_type=F32)
            return gelu(acc + b_in[:, pl.ds(c * COLS, COLS)]).astype(BF16), jnp.minimum(jnp.abs(acc[:, :LANES]), 0.0)

        def put(dst, c, value):
            for j in range(per):
                for k in range(2):
                    dst[c * per + j, pl.ds(starts[k], half), :] = value[k * half:(k + 1) * half, j * LANES:(j + 1) * LANES]

        if first:
            for j in range(gate_tiles, 2 * gate_tiles):
                wi_copy(j).wait()
        for c in range(n_cols):
            value, _ = chunk(n_cols + c)
            put(vn, c, value)
            value = value.astype(F32)
            tiles = [value[:, j * LANES:(j + 1) * LANES] for j in range(per)]
            if c == 0:
                pivot = tiles[0]
                stat[0] = pivot
                tiles = tiles[1:]
            else:
                pivot = stat[0]
            diffs = [v - pivot for v in tiles]
            total = sum(diffs[1:], diffs[0])
            squares = sum([d * d for d in diffs[1:]], diffs[0] * diffs[0])
            stat[1] = total if c == 0 else stat[1] + total
            stat[2] = squares if c == 0 else stat[2] + squares
        if first:
            for j in range(gate_tiles):
                wi_copy(j).wait()
        total = stat[1]
        mean_lane = stat[0] + total * (1.0 / gate_tiles)
        mean = jnp.sum(mean_lane, axis=-1, keepdims=True) * (1.0 / LANES)
        away = mean_lane - mean
        spread = (stat[2] - total * total * (1.0 / gate_tiles)) + gate_tiles * (away * away)
        var = jnp.maximum(jnp.sum(spread, axis=-1, keepdims=True) * (1.0 / gate), 0.0)
        stat[0] = jnp.broadcast_to(mean, (rows, LANES))
        stat[1] = jnp.broadcast_to(lax.rsqrt(var + LN_EPS), (rows, LANES))

        def norm(j, mean_now):
            for k in range(2):
                part = pl.ds(starts[k], half)
                here = pl.ds(k * half, half)
                value = (vn[j, part, :].astype(F32) - mean_now[k * half:(k + 1) * half]) * stat[1, here]
                vn[j, part, :] = (value * ln2s[:, lanes(j)] + ln2b[:, lanes(j)]).astype(BF16)

        for c in range(n_cols):
            value, zero = chunk(c)
            put(g, c, value)
            mean_now = stat[0] + zero
            for j in range(c * per, (c + 1) * per):
                norm(j, mean_now)

    def stage_b(i):
        at = pl.ds(i * rows, rows)
        depth = (i + 1) * rows
        for j in range(depth // LANES):
            ws[j, at, :] = jnp.where(mk[at, lanes(j)] > 0, ws[j, at, :].astype(F32), 0.0).astype(BF16)
        for c in range(n_cols):
            tiles = range(c * per, (c + 1) * per)
            s = jnp.dot(wide(ws, range(depth // LANES), at), wide(vn, tiles, pl.ds(0, depth)), preferred_element_type=F32)
            for j in range(per):
                t = (s[:, j * LANES:(j + 1) * LANES] + bias[at, :]).astype(BF16).astype(F32)
                q[tiles[j]] = (g[tiles[j], at, :].astype(F32) * t).astype(BF16)
        for c in range(width // COLS):
            cols = pl.ds(c * COLS, COLS)
            y = jnp.dot(wide(q, range(gate_tiles)), wide(wo, range(c * per, (c + 1) * per)), preferred_element_type=F32)
            ybuf[i, :, cols] = (xbuf[i, :, cols].astype(F32) + (y + b_out[:, cols])).astype(BF16)

    stage_a(0, True)
    even0 = (1 - chip) * (1 - core)
    odd0 = (1 - chip) * core

    def outer(k, carry):
        def upto(k):
            return n - 2 * odd0 * (1 - k // 2)

        def one(t, c):
            stage_a(t, False)
            return c

        lax.fori_loop(jnp.where(k == 0, 1, upto(k - 1)), upto(k), one, 0)

        @pl.when(k == 0)
        def _():
            for j in range(length // LANES):
                ws_copy(j).wait()
            mk_copy().wait()
            for j in range(width // LANES):
                wo_copy(j).wait()

        block = lax.rem(k + 2 * even0, n)
        for i in range(n):
            pl.when(block == i)(functools.partial(stage_b, i))

        @pl.when(me == block)
        def _():
            y_own().start()

        @pl.when(me != block)
        def _():
            y_send(block).start()

        return carry

    lax.fori_loop(0, n, outer, 0)

    for k in range(1, n):
        peer = lax.rem(me + k, n)
        for p in range(2):
            x_send(peer, p).wait_send()
        y_send(peer).wait_send()
        y_recv(peer).wait_recv()
    y_own().wait()


def solution(mesh):
    n = mesh.shape["seq"]
    row_spec = P("data", "seq", None)

    def local_block(act_in, ln1_scale, ln1_bias, w_in, b_in, ln2_scale, ln2_bias, w_spatial, b_spatial, causal_mask, w_out, b_out):
        rows, width = act_in.shape[1:]
        length = n * rows
        gate = w_out.shape[0]
        hbm = pl.BlockSpec(memory_space=pl.ANY)
        vmem = pl.BlockSpec(memory_space=pltpu.VMEM)

        def row(v):
            return v.reshape(1, -1)

        return pl.pallas_call(
            functools.partial(body, n),
            out_shape=jax.ShapeDtypeStruct(act_in.shape, act_in.dtype),
            in_specs=[hbm, vmem, vmem, hbm, vmem, vmem, vmem, hbm, vmem, hbm, hbm, vmem],
            out_specs=hbm,
            scratch_shapes=[
                pltpu.VMEM((n, rows, width), BF16),
                pltpu.VMEM((2 * gate // LANES, width, LANES), BF16),
                pltpu.VMEM((width // LANES, gate, LANES), BF16),
                pltpu.VMEM((length // LANES, length, LANES), BF16),
                pltpu.VMEM((length, length), jnp.int32),
                pltpu.VMEM((gate // LANES, length, LANES), BF16),
                pltpu.VMEM((gate // LANES, length, LANES), BF16),
                pltpu.VMEM((width // LANES, rows, LANES), BF16),
                pltpu.VMEM((gate // LANES, rows, LANES), BF16),
                pltpu.VMEM((n, rows, width), BF16),
                pltpu.VMEM((length, LANES), F32),
                pltpu.VMEM((3, rows, LANES), F32),
                pltpu.SemaphoreType.DMA((n, 2)),
                pltpu.SemaphoreType.DMA((n, 2)),
                pltpu.SemaphoreType.DMA((n,)),
                pltpu.SemaphoreType.DMA((n,)),
                pltpu.SemaphoreType.DMA((2 * gate // LANES,)),
                pltpu.SemaphoreType.DMA((width // LANES,)),
                pltpu.SemaphoreType.DMA((length // LANES,)),
                pltpu.SemaphoreType.DMA,
            ],
            compiler_params=pltpu.CompilerParams(
                collective_id=0, has_side_effects=True, vmem_limit_bytes=60 * 1024 * 1024),
            name="gmlp",
        )(act_in, row(ln1_scale), row(ln1_bias), w_in, row(b_in), row(ln2_scale), row(ln2_bias),
          w_spatial, row(b_spatial), causal_mask, w_out, row(b_out))

    return jax.shard_map(local_block, mesh=mesh, in_specs=(row_spec,) + (P(),) * 11, out_specs=row_spec, check_vma=False)
```

```python
import functools

import jax
import jax.numpy as jnp
from jax import lax
from jax.experimental import pallas as pl
from jax.experimental.pallas import tpu as pltpu
from jax.sharding import PartitionSpec as P

LN_EPS = 1e-6
GELU_A = 0.7978845608028654
GELU_B = GELU_A * 0.044715
COLS = 512
LANES = 128
MESH = pl.DeviceIdType.MESH
F32 = jnp.float32
BF16 = jnp.bfloat16


def gelu(a):
    return a * jax.nn.sigmoid(a * (2 * GELU_A + 2 * GELU_B * (a * a)))


def layer_norm(x, gain, shift):
    width = x.shape[-1]
    mean = jnp.sum(x, axis=-1, keepdims=True) * (1.0 / width)
    centered = x - mean
    var = jnp.sum(centered * centered, axis=-1, keepdims=True) * (1.0 / width)
    return centered * lax.rsqrt(var + LN_EPS) * gain + shift


def wide(ref, tiles, *where):
    return jnp.concatenate([ref[(j, *where)] for j in tiles], axis=1)


def body(n, act, ln1s, ln1b, w_in, b_in, ln2s, ln2b, w_sp, b_sp, mask, w_out, b_out, out,
         xbuf, wi, wo, ws, mk, vn, g, u, q, ybuf, bias, stat,
         xs_sem, xr_sem, ys_sem, yr_sem, wi_sem, wo_sem, ws_sem, mk_sem):
    me = lax.axis_index("seq")
    chip, core = me // 2, lax.rem(me, 2)
    partner = chip * 2 + 1 - core
    far = (1 - chip) * 2
    rows, width = act.shape[1], act.shape[2]
    length = n * rows
    half = rows // 2
    gate = w_out.shape[0]
    gate_tiles = gate // LANES
    n_cols = gate // COLS
    per = COLS // LANES

    def lanes(j):
        return pl.ds(j * LANES, LANES)

    def wi_copy(j):
        return pltpu.make_async_copy(w_in.at[:, lanes(j)], wi.at[j], wi_sem.at[j])

    def ws_copy(j):
        return pltpu.make_async_copy(w_sp.at[:, lanes(j)], ws.at[j], ws_sem.at[j])

    def wo_copy(j):
        return pltpu.make_async_copy(w_out.at[:, lanes(j)], wo.at[j], wo_sem.at[j])

    def mk_copy():
        return pltpu.make_async_copy(mask, mk, mk_sem)

    def own_x(p):
        part = pl.ds(p * half, half)
        return pltpu.make_async_copy(act.at[me, part], xbuf.at[me, part], xr_sem.at[me, p])

    def x_send(dest, p):
        part = pl.ds(p * half, half)
        return pltpu.make_async_remote_copy(
            src_ref=act.at[dest, part], dst_ref=xbuf.at[me, part], send_sem=xs_sem.at[dest, p], recv_sem=xr_sem.at[me, p],
            device_id={"seq": dest}, device_id_type=MESH)

    def x_recv(block, p):
        part = pl.ds(p * half, half)
        return pltpu.make_async_remote_copy(
            src_ref=act.at[block, part], dst_ref=xbuf.at[block, part], send_sem=xs_sem.at[block, p],
            recv_sem=xr_sem.at[block, p], device_id={"seq": block}, device_id_type=MESH)

    def y_send(block):
        return pltpu.make_async_remote_copy(
            src_ref=ybuf.at[block], dst_ref=out.at[me], send_sem=ys_sem.at[block], recv_sem=yr_sem.at[me],
            device_id={"seq": block}, device_id_type=MESH)

    def y_recv(block):
        return pltpu.make_async_remote_copy(
            src_ref=ybuf.at[block], dst_ref=out.at[block], send_sem=ys_sem.at[block], recv_sem=yr_sem.at[block],
            device_id={"seq": block}, device_id_type=MESH)

    def y_own():
        return pltpu.make_async_copy(ybuf.at[me], out.at[me], yr_sem.at[me])

    barrier = pltpu.get_barrier_semaphore()
    for k in range(1, n):
        pl.semaphore_signal(barrier, inc=1, device_id={"seq": lax.rem(me + k, n)}, device_id_type=MESH)
    for p in range(2):
        own_x(p).start()
    for j in range(2 * gate_tiles):
        wi_copy((j + gate_tiles) % (2 * gate_tiles)).start()
    pl.semaphore_wait(barrier, n - 1)
    for dest in (far, partner, far + 1):
        for p in range(2):
            x_send(dest, p).start()
    for j in range(length // LANES):
        ws_copy(j).start()
    mk_copy().start()
    for j in range(width // LANES):
        wo_copy(j).start()

    for i in range(n):
        at = pl.ds(i * rows, rows)
        bias[at, :] = jnp.broadcast_to(b_sp[:, at], (LANES, rows)).T

    def stage_a(t, first):
        if first:
            pieces = [(me, 0), (me, 1)]
            for p in range(2):
                own_x(p).wait()
        else:
            remote = t // 2
            side = t - 2
            pieces = [((1 - remote) * partner + remote * far, remote * side),
                      ((1 - remote) * partner + remote * (far + 1), (1 - remote) + remote * side)]
            for block, p in pieces:
                x_recv(block, p).wait_recv()
        starts = [pl.multiple_of(block * rows + p * half, half) for block, p in pieces]
        step1 = 64
        for k, (block, p) in enumerate(pieces):
            for r in range(half // step1):
                x = xbuf[block, pl.ds(pl.multiple_of(p * half, half) + r * step1, step1), :].astype(F32)
                x = layer_norm(x, ln1s[...], ln1b[...]).astype(BF16)
                for j in range(width // LANES):
                    u[j, pl.ds(k * half + r * step1, step1), :] = x[:, j * LANES:(j + 1) * LANES]

        def chunk(c):
            tiles = range(c * per, (c + 1) * per)
            acc = jnp.dot(wide(u, range(width // LANES)), wide(wi, tiles), preferred_element_type=F32)
            return gelu(acc + b_in[:, pl.ds(c * COLS, COLS)]).astype(BF16), jnp.minimum(jnp.abs(acc[:, :LANES]), 0.0)

        def put(dst, c, value):
            for j in range(per):
                for k in range(2):
                    dst[c * per + j, pl.ds(starts[k], half), :] = value[k * half:(k + 1) * half, j * LANES:(j + 1) * LANES]

        if first:
            for j in range(gate_tiles, 2 * gate_tiles):
                wi_copy(j).wait()
        for c in range(n_cols):
            value, _ = chunk(n_cols + c)
            put(vn, c, value)
            value = value.astype(F32)
            tiles = [value[:, j * LANES:(j + 1) * LANES] for j in range(per)]
            if c == 0:
                pivot = tiles[0]
                stat[0] = pivot
                tiles = tiles[1:]
            else:
                pivot = stat[0]
            diffs = [v - pivot for v in tiles]
            total = sum(diffs[1:], diffs[0])
            squares = sum([d * d for d in diffs[1:]], diffs[0] * diffs[0])
            stat[1] = total if c == 0 else stat[1] + total
            stat[2] = squares if c == 0 else stat[2] + squares
        if first:
            for j in range(gate_tiles):
                wi_copy(j).wait()
        total = stat[1]
        mean_lane = stat[0] + total * (1.0 / gate_tiles)
        mean = jnp.sum(mean_lane, axis=-1, keepdims=True) * (1.0 / LANES)
        away = mean_lane - mean
        spread = (stat[2] - total * total * (1.0 / gate_tiles)) + gate_tiles * (away * away)
        var = jnp.maximum(jnp.sum(spread, axis=-1, keepdims=True) * (1.0 / gate), 0.0)
        stat[0] = jnp.broadcast_to(mean, (rows, LANES))
        stat[1] = jnp.broadcast_to(lax.rsqrt(var + LN_EPS), (rows, LANES))

        def norm(j, mean_now):
            for k in range(2):
                part = pl.ds(starts[k], half)
                here = pl.ds(k * half, half)
                value = (vn[j, part, :].astype(F32) - mean_now[k * half:(k + 1) * half]) * stat[1, here]
                vn[j, part, :] = (value * ln2s[:, lanes(j)] + ln2b[:, lanes(j)]).astype(BF16)

        for c in range(n_cols):
            value, zero = chunk(c)
            put(g, c, value)
            mean_now = stat[0] + zero
            for j in range(c * per, (c + 1) * per):
                norm(j, mean_now)

    def stage_b(i):
        at = pl.ds(i * rows, rows)
        depth = (i + 1) * rows
        for j in range(depth // LANES):
            ws[j, at, :] = jnp.where(mk[at, lanes(j)] > 0, ws[j, at, :].astype(F32), 0.0).astype(BF16)
        for c in range(n_cols):
            tiles = range(c * per, (c + 1) * per)
            s = jnp.dot(wide(ws, range(depth // LANES), at), wide(vn, tiles, pl.ds(0, depth)), preferred_element_type=F32)
            for j in range(per):
                t = (s[:, j * LANES:(j + 1) * LANES] + bias[at, :]).astype(BF16).astype(F32)
                q[tiles[j]] = (g[tiles[j], at, :].astype(F32) * t).astype(BF16)
        for c in range(width // COLS):
            cols = pl.ds(c * COLS, COLS)
            y = jnp.dot(wide(q, range(gate_tiles)), wide(wo, range(c * per, (c + 1) * per)), preferred_element_type=F32)
            ybuf[i, :, cols] = (xbuf[i, :, cols].astype(F32) + (y + b_out[:, cols])).astype(BF16)

    stage_a(0, True)
    even0 = (1 - chip) * (1 - core)
    odd0 = (1 - chip) * core

    def outer(k, carry):
        def upto(k):
            return n - 2 * odd0 * (1 - k // 2)

        def one(t, c):
            stage_a(t, False)
            return c

        lax.fori_loop(jnp.where(k == 0, 1, upto(k - 1)), upto(k), one, 0)

        @pl.when(k == 0)
        def _():
            for j in range(length // LANES):
                ws_copy(j).wait()
            mk_copy().wait()
            for j in range(width // LANES):
                wo_copy(j).wait()

        block = lax.rem(k + 2 * even0, n)
        for i in range(n):
            pl.when(block == i)(functools.partial(stage_b, i))

        @pl.when(me == block)
        def _():
            y_own().start()

        @pl.when(me != block)
        def _():
            y_send(block).start()

        return carry

    lax.fori_loop(0, n, outer, 0)

    for k in range(1, n):
        peer = lax.rem(me + k, n)
        for p in range(2):
            x_send(peer, p).wait_send()
        y_send(peer).wait_send()
        y_recv(peer).wait_recv()
    y_own().wait()


def solution(mesh):
    n = mesh.shape["seq"]
    row_spec = P("data", "seq", None)

    def local_block(act_in, ln1_scale, ln1_bias, w_in, b_in, ln2_scale, ln2_bias, w_spatial, b_spatial, causal_mask, w_out, b_out):
        rows, width = act_in.shape[1:]
        length = n * rows
        gate = w_out.shape[0]
        hbm = pl.BlockSpec(memory_space=pl.ANY)
        vmem = pl.BlockSpec(memory_space=pltpu.VMEM)

        def row(v):
            return v.reshape(1, -1)

        return pl.pallas_call(
            functools.partial(body, n),
            out_shape=pltpu.VMEM(act_in.shape, act_in.dtype),
            in_specs=[hbm, vmem, vmem, hbm, vmem, vmem, vmem, hbm, vmem, hbm, hbm, vmem],
            out_specs=hbm,
            scratch_shapes=[
                pltpu.VMEM((n, rows, width), BF16),
                pltpu.VMEM((2 * gate // LANES, width, LANES), BF16),
                pltpu.VMEM((width // LANES, gate, LANES), BF16),
                pltpu.VMEM((length // LANES, length, LANES), BF16),
                pltpu.VMEM((length, length), jnp.int32),
                pltpu.VMEM((gate // LANES, length, LANES), BF16),
                pltpu.VMEM((gate // LANES, length, LANES), BF16),
                pltpu.VMEM((width // LANES, rows, LANES), BF16),
                pltpu.VMEM((gate // LANES, rows, LANES), BF16),
                pltpu.VMEM((n, rows, width), BF16),
                pltpu.VMEM((length, LANES), F32),
                pltpu.VMEM((3, rows, LANES), F32),
                pltpu.SemaphoreType.DMA((n, 2)),
                pltpu.SemaphoreType.DMA((n, 2)),
                pltpu.SemaphoreType.DMA((n,)),
                pltpu.SemaphoreType.DMA((n,)),
                pltpu.SemaphoreType.DMA((2 * gate // LANES,)),
                pltpu.SemaphoreType.DMA((width // LANES,)),
                pltpu.SemaphoreType.DMA((length // LANES,)),
                pltpu.SemaphoreType.DMA,
            ],
            compiler_params=pltpu.CompilerParams(
                collective_id=0, has_side_effects=True, vmem_limit_bytes=60 * 1024 * 1024),
            name="gmlp",
        )(act_in, row(ln1_scale), row(ln1_bias), w_in, row(b_in), row(ln2_scale), row(ln2_bias),
          w_spatial, row(b_spatial), causal_mask, w_out, row(b_out))

    return jax.shard_map(local_block, mesh=mesh, in_specs=(row_spec,) + (P(),) * 11, out_specs=row_spec, check_vma=False)
```

```python
import functools

import jax
import jax.numpy as jnp
from jax import lax
from jax.experimental import pallas as pl
from jax.experimental.pallas import tpu as pltpu
from jax.sharding import PartitionSpec as P

LN_EPS = 1e-6
GELU_A = 0.7978845608028654
GELU_B = GELU_A * 0.044715
COLS = 512
LANES = 128
MESH = pl.DeviceIdType.MESH
F32 = jnp.float32
BF16 = jnp.bfloat16


def gelu(a):
    return a * jax.nn.sigmoid(a * (2 * GELU_A + 2 * GELU_B * (a * a)))


def layer_norm(x, gain, shift):
    width = x.shape[-1]
    mean = jnp.sum(x, axis=-1, keepdims=True) * (1.0 / width)
    centered = x - mean
    var = jnp.sum(centered * centered, axis=-1, keepdims=True) * (1.0 / width)
    return centered * lax.rsqrt(var + LN_EPS) * gain + shift


def wide(ref, tiles, *where):
    return jnp.concatenate([ref[(j, *where)] for j in tiles], axis=1)


def body(n, act, ln1s_hbm, ln1b_hbm, w_in, b_in_hbm, ln2s_hbm, ln2b_hbm, w_sp, b_sp_hbm, mask, w_out, b_out_hbm, out,
         ln1s, ln1b, b_in, ln2s, ln2b, b_sp, b_out, xbuf, wi, wo, ws, mk, vn, g, u, q, ybuf, bias, stat,
         xs_sem, xr_sem, ys_sem, yr_sem, wi_sem, wo_sem, ws_sem, mk_sem, vec_sem):
    me = lax.axis_index("seq")
    chip, core = me // 2, lax.rem(me, 2)
    partner = chip * 2 + 1 - core
    far = (1 - chip) * 2
    even0 = (1 - chip) * (1 - core)
    odd0 = (1 - chip) * core
    rows, width = act.shape[1], act.shape[2]
    length = n * rows
    half = rows // 2
    gate = w_out.shape[0]
    gate_tiles = gate // LANES
    n_cols = gate // COLS
    per = COLS // LANES

    def lanes(j):
        return pl.ds(j * LANES, LANES)

    def wi_copy(j):
        return pltpu.make_async_copy(w_in.at[:, lanes(j)], wi.at[j], wi_sem.at[j])

    def ws_copy(j):
        return pltpu.make_async_copy(w_sp.at[:, lanes(j)], ws.at[j], ws_sem.at[j])

    def wo_copy(j):
        return pltpu.make_async_copy(w_out.at[:, lanes(j)], wo.at[j], wo_sem.at[j])

    def mk_copy():
        return pltpu.make_async_copy(mask, mk, mk_sem)

    def own_x(p):
        part = pl.ds(p * half, half)
        return pltpu.make_async_copy(act.at[me, part], xbuf.at[me, part], xr_sem.at[me, p])

    def x_send(dest, p):
        part = pl.ds(p * half, half)
        return pltpu.make_async_remote_copy(
            src_ref=act.at[dest, part], dst_ref=xbuf.at[me, part], send_sem=xs_sem.at[dest, p], recv_sem=xr_sem.at[me, p],
            device_id={"seq": dest}, device_id_type=MESH)

    def x_recv(block, p):
        part = pl.ds(p * half, half)
        return pltpu.make_async_remote_copy(
            src_ref=act.at[partner, part], dst_ref=xbuf.at[block, part], send_sem=xs_sem.at[block, p],
            recv_sem=xr_sem.at[block, p], device_id={"seq": partner}, device_id_type=MESH)

    def extra_own(p):
        part = pl.ds(p * half, half)
        return pltpu.make_async_copy(act.at[far, part], xbuf.at[n, part], xr_sem.at[n, p])

    def extra_send(p):
        part = pl.ds(p * half, half)
        return pltpu.make_async_remote_copy(
            src_ref=act.at[far + 1, part], dst_ref=xbuf.at[n, part], send_sem=xs_sem.at[n, p], recv_sem=xr_sem.at[n, p],
            device_id={"seq": partner}, device_id_type=MESH)

    def y_send(slot):
        extra = slot // n
        seq = (1 - extra) * me + extra * (far + core)
        return pltpu.make_async_remote_copy(
            src_ref=ybuf.at[slot], dst_ref=out.at[seq], send_sem=ys_sem.at[slot], recv_sem=yr_sem.at[seq],
            device_id={"seq": slot - extra * n}, device_id_type=MESH)

    def y_recv(block):
        return pltpu.make_async_remote_copy(
            src_ref=ybuf.at[block], dst_ref=out.at[block], send_sem=ys_sem.at[block], recv_sem=yr_sem.at[block],
            device_id={"seq": block}, device_id_type=MESH)

    def y_own(slot):
        extra = slot // n
        seq = (1 - extra) * me + extra * (far + core)
        return pltpu.make_async_copy(ybuf.at[slot], out.at[seq], yr_sem.at[seq])

    vectors = [pltpu.make_async_copy(src, dst, vec_sem.at[k]) for k, (src, dst) in enumerate((
        (ln1s_hbm, ln1s), (ln1b_hbm, ln1b), (b_sp_hbm, b_sp), (b_in_hbm, b_in), (ln2s_hbm, ln2s), (ln2b_hbm, ln2b),
        (b_out_hbm, b_out)))]

    barrier = pltpu.get_barrier_semaphore()
    for k in range(1, n):
        pl.semaphore_signal(barrier, inc=1, device_id={"seq": lax.rem(me + k, n)}, device_id_type=MESH)
    for p in range(2):
        own_x(p).start()
    for copy in vectors:
        copy.start()
    for j in range(2 * gate_tiles):
        wi_copy((j + gate_tiles) % (2 * gate_tiles)).start()
    pl.semaphore_wait(barrier, n - 1)
    for dest in (far, partner, far + 1):
        for p in range(2):
            x_send(dest, p).start()
    @pl.when(me == 0)
    def _():
        for p in range(2):
            extra_send(p).start()
            extra_own(p).start()

    for j in range(length // LANES):
        ws_copy(j).start()
    mk_copy().start()
    for j in range(width // LANES):
        wo_copy(j).start()

    for copy in vectors:
        copy.wait()
    for i in range(n):
        at = pl.ds(i * rows, rows)
        bias[at, :] = jnp.broadcast_to(b_sp[:, at], (LANES, rows)).T

    def stage_a(t, first):
        if first:
            pieces = [(me, 0), (me, 1)]
            for p in range(2):
                own_x(p).wait()
        else:
            near, extra = 1 - (t + 2) // 4, t // 4
            remote = 1 - near - extra
            side = t - 2
            pieces = [
                (near * partner + remote * (far + even0 * side) + extra * n, remote * (1 - even0) * side),
                (near * partner + remote * (far + even0 * side + (1 - even0)) + extra * n,
                 near + extra + remote * (even0 + (1 - even0) * side))]

            @pl.when(extra * (1 - core) == 1)
            def _():
                for p in range(2):
                    extra_own(p).wait()

            @pl.when(extra * (1 - core) == 0)
            def _():
                for block, p in pieces:
                    x_recv(block, p).wait_recv()

        starts = [pl.multiple_of(lax.rem(block, n) * rows + p * half, half) for block, p in pieces]
        step1 = 64
        for k, (block, p) in enumerate(pieces):
            for r in range(half // step1):
                x = xbuf[block, pl.ds(pl.multiple_of(p * half, half) + r * step1, step1), :].astype(F32)
                x = layer_norm(x, ln1s[...], ln1b[...]).astype(BF16)
                for j in range(width // LANES):
                    u[j, pl.ds(k * half + r * step1, step1), :] = x[:, j * LANES:(j + 1) * LANES]

        def chunk(c):
            tiles = range(c * per, (c + 1) * per)
            acc = jnp.dot(wide(u, range(width // LANES)), wide(wi, tiles), preferred_element_type=F32)
            return gelu(acc + b_in[:, pl.ds(c * COLS, COLS)]).astype(BF16), jnp.minimum(jnp.abs(acc[:, :LANES]), 0.0)

        def put(dst, c, value):
            for j in range(per):
                for k in range(2):
                    dst[c * per + j, pl.ds(starts[k], half), :] = value[k * half:(k + 1) * half, j * LANES:(j + 1) * LANES]

        if first:
            for j in range(gate_tiles, 2 * gate_tiles):
                wi_copy(j).wait()
        for c in range(n_cols):
            value, _ = chunk(n_cols + c)
            put(vn, c, value)
            value = value.astype(F32)
            tiles = [value[:, j * LANES:(j + 1) * LANES] for j in range(per)]
            if c == 0:
                pivot = tiles[0]
                stat[0] = pivot
                tiles = tiles[1:]
            else:
                pivot = stat[0]
            diffs = [v - pivot for v in tiles]
            total = sum(diffs[1:], diffs[0])
            squares = sum([d * d for d in diffs[1:]], diffs[0] * diffs[0])
            stat[1] = total if c == 0 else stat[1] + total
            stat[2] = squares if c == 0 else stat[2] + squares
        if first:
            for j in range(gate_tiles):
                wi_copy(j).wait()
        total = stat[1]
        mean_lane = stat[0] + total * (1.0 / gate_tiles)
        mean = jnp.sum(mean_lane, axis=-1, keepdims=True) * (1.0 / LANES)
        away = mean_lane - mean
        spread = (stat[2] - total * total * (1.0 / gate_tiles)) + gate_tiles * (away * away)
        var = jnp.maximum(jnp.sum(spread, axis=-1, keepdims=True) * (1.0 / gate), 0.0)
        stat[0] = jnp.broadcast_to(mean, (rows, LANES))
        stat[1] = jnp.broadcast_to(lax.rsqrt(var + LN_EPS), (rows, LANES))

        def norm(j, mean_now):
            for k in range(2):
                part = pl.ds(starts[k], half)
                here = pl.ds(k * half, half)
                value = (vn[j, part, :].astype(F32) - mean_now[k * half:(k + 1) * half]) * stat[1, here]
                vn[j, part, :] = (value * ln2s[:, lanes(j)] + ln2b[:, lanes(j)]).astype(BF16)

        for c in range(n_cols):
            value, zero = chunk(c)
            put(g, c, value)
            mean_now = stat[0] + zero
            for j in range(c * per, (c + 1) * per):
                norm(j, mean_now)

    def stage_b(slot, i):
        at = pl.ds(i * rows, rows)
        depth = (i + 1) * rows
        for j in range(depth // LANES):
            ws[j, at, :] = jnp.where(mk[at, lanes(j)] > 0, ws[j, at, :].astype(F32), 0.0).astype(BF16)
        for c in range(n_cols):
            tiles = range(c * per, (c + 1) * per)
            s = jnp.dot(wide(ws, range(depth // LANES), at), wide(vn, tiles, pl.ds(0, depth)), preferred_element_type=F32)
            for j in range(per):
                t = (s[:, j * LANES:(j + 1) * LANES] + bias[at, :]).astype(BF16).astype(F32)
                q[tiles[j]] = (g[tiles[j], at, :].astype(F32) * t).astype(BF16)
        for c in range(width // COLS):
            cols = pl.ds(c * COLS, COLS)
            y = jnp.dot(wide(q, range(gate_tiles)), wide(wo, range(c * per, (c + 1) * per)), preferred_element_type=F32)
            ybuf[slot, :, cols] = (xbuf[slot, :, cols].astype(F32) + (y + b_out[:, cols])).astype(BF16)

    stage_a(0, True)

    def outer(k, carry):
        last = k // n
        def upto(k):
            return (even0 * (3 + (k + 3) // 4 + k // 4) + odd0 * (2 + 2 * ((k + 2) // 4) + k // 4) + chip * n)

        def one(t, c):
            stage_a(t, False)
            return c

        lax.fori_loop(jnp.where(k == 0, 1, upto(k - 1)), upto(k), one, 0)

        @pl.when(k == 0)
        def _():
            for j in range(length // LANES):
                ws_copy(j).wait()
            mk_copy().wait()
            for j in range(width // LANES):
                wo_copy(j).wait()

        slot = even0 * ((1 - last) * lax.rem(k + 2, n) + last * n) + odd0 * k + chip * (k + 1)
        block = lax.rem(slot, n)
        for i in range(n):
            pl.when(block == i)(functools.partial(stage_b, slot, i))

        @pl.when(me == block)
        def _():
            y_own(slot).start()

        @pl.when(me != block)
        def _():
            y_send(slot).start()

        return carry

    lax.fori_loop(0, (1 - chip) * (n + 1) + chip * (n - 1), outer, 0)

    for k in range(1, n):
        for p in range(2):
            x_send(lax.rem(me + k, n), p).wait_send()

    @pl.when(me == 0)
    def _():
        for p in range(2):
            extra_send(p).wait_send()
        y_own(n).wait()

    @pl.when(me == 1)
    def _():
        y_send(n).wait_send()

    @pl.when((me != 0) & (chip == 0))
    def _():
        y_send(0).wait_send()

    for block in range(1, n):
        @pl.when(me != block)
        def _():
            y_send(block).wait_send()

    for seq in range(n):
        @pl.when((me != seq) & ((me != 0) | (seq != 2)))
        def _():
            y_recv(seq).wait_recv()

    y_own(me).wait()


def solution(mesh):
    n = mesh.shape["seq"]
    row_spec = P("data", "seq", None)

    def local_block(act_in, ln1_scale, ln1_bias, w_in, b_in, ln2_scale, ln2_bias, w_spatial, b_spatial, causal_mask, w_out, b_out):
        rows, width = act_in.shape[1:]
        length = n * rows
        gate = w_out.shape[0]
        hbm = pl.BlockSpec(memory_space=pl.ANY)

        def row(v):
            return v.reshape(1, -1)

        return pl.pallas_call(
            functools.partial(body, n),
            out_shape=pltpu.VMEM(act_in.shape, act_in.dtype),
            in_specs=[hbm] * 12,
            out_specs=hbm,
            scratch_shapes=[
                pltpu.VMEM((1, width), F32),
                pltpu.VMEM((1, width), F32),
                pltpu.VMEM((1, 2 * gate), F32),
                pltpu.VMEM((1, gate), F32),
                pltpu.VMEM((1, gate), F32),
                pltpu.VMEM((1, length), F32),
                pltpu.VMEM((1, width), F32),
                pltpu.VMEM((n + 1, rows, width), BF16),
                pltpu.VMEM((2 * gate // LANES, width, LANES), BF16),
                pltpu.VMEM((width // LANES, gate, LANES), BF16),
                pltpu.VMEM((length // LANES, length, LANES), BF16),
                pltpu.VMEM((length, length), jnp.int32),
                pltpu.VMEM((gate // LANES, length, LANES), BF16),
                pltpu.VMEM((gate // LANES, length, LANES), BF16),
                pltpu.VMEM((width // LANES, rows, LANES), BF16),
                pltpu.VMEM((gate // LANES, rows, LANES), BF16),
                pltpu.VMEM((n + 1, rows, width), BF16),
                pltpu.VMEM((length, LANES), F32),
                pltpu.VMEM((3, rows, LANES), F32),
                pltpu.SemaphoreType.DMA((n + 1, 2)),
                pltpu.SemaphoreType.DMA((n + 1, 2)),
                pltpu.SemaphoreType.DMA((n + 1,)),
                pltpu.SemaphoreType.DMA((n,)),
                pltpu.SemaphoreType.DMA((2 * gate // LANES,)),
                pltpu.SemaphoreType.DMA((width // LANES,)),
                pltpu.SemaphoreType.DMA((length // LANES,)),
                pltpu.SemaphoreType.DMA,
                pltpu.SemaphoreType.DMA((7,)),
            ],
            compiler_params=pltpu.CompilerParams(
                collective_id=0, has_side_effects=True, vmem_limit_bytes=60 * 1024 * 1024),
            name="gmlp",
        )(act_in, row(ln1_scale), row(ln1_bias), w_in, row(b_in), row(ln2_scale), row(ln2_bias),
          w_spatial, row(b_spatial), causal_mask, w_out, row(b_out))

    return jax.shard_map(local_block, mesh=mesh, in_specs=(row_spec,) + (P(),) * 11, out_specs=row_spec, check_vma=False)
```

```python
import functools

import jax
import jax.numpy as jnp
from jax import lax
from jax.experimental import pallas as pl
from jax.experimental.pallas import tpu as pltpu
from jax.sharding import PartitionSpec as P

LN_EPS = 1e-6
GELU_A = 0.7978845608028654
GELU_B = GELU_A * 0.044715
COLS = 512
LANES = 128
MESH = pl.DeviceIdType.MESH
F32 = jnp.float32
BF16 = jnp.bfloat16


def gelu(a):
    return a * jax.nn.sigmoid(a * (2 * GELU_A + 2 * GELU_B * (a * a)))


def layer_norm(x, gain, shift):
    width = x.shape[-1]
    mean = jnp.sum(x, axis=-1, keepdims=True) * (1.0 / width)
    centered = x - mean
    var = jnp.sum(centered * centered, axis=-1, keepdims=True) * (1.0 / width)
    return centered * lax.rsqrt(var + LN_EPS) * gain + shift


def wide(ref, tiles, *where):
    return jnp.concatenate([ref[(j, *where)] for j in tiles], axis=1)


def body(n, act, ln1s_hbm, ln1b_hbm, w_in, b_in_hbm, ln2s_hbm, ln2b_hbm, w_sp, b_sp_hbm, mask, w_out, b_out_hbm, out,
         ln1s, ln1b, b_in, ln2s, ln2b, b_sp, b_out, xbuf, wi, wo, ws, mk, vn, g, u, q, ybuf, bias, stat,
         xs_sem, xr_sem, ys_sem, yr_sem, wi_sem, wo_sem, ws_sem, mk_sem, vec_sem):
    me = lax.axis_index("seq")
    chip, core = me // 2, lax.rem(me, 2)
    partner = chip * 2 + 1 - core
    far = (1 - chip) * 2
    even0 = (1 - chip) * (1 - core)
    odd0 = (1 - chip) * core
    rows, width = act.shape[1], act.shape[2]
    length = n * rows
    half = rows // 2
    gate = w_out.shape[0]
    gate_tiles = gate // LANES
    n_cols = gate // COLS
    per = COLS // LANES

    def lanes(j):
        return pl.ds(j * LANES, LANES)

    def wi_copy(j):
        return pltpu.make_async_copy(w_in.at[:, lanes(j)], wi.at[j], wi_sem.at[j])

    def ws_copy(j):
        return pltpu.make_async_copy(w_sp.at[:, lanes(j)], ws.at[j], ws_sem.at[j])

    def wo_copy(j):
        return pltpu.make_async_copy(w_out.at[:, lanes(j)], wo.at[j], wo_sem.at[j])

    def mk_copy():
        return pltpu.make_async_copy(mask, mk, mk_sem)

    def own_x(p):
        part = pl.ds(p * half, half)
        return pltpu.make_async_copy(act.at[me, part], xbuf.at[me, part], xr_sem.at[me, p])

    def x_send(dest, p):
        part = pl.ds(p * half, half)
        return pltpu.make_async_remote_copy(
            src_ref=act.at[dest, part], dst_ref=xbuf.at[me, part], send_sem=xs_sem.at[dest, p], recv_sem=xr_sem.at[me, p],
            device_id={"seq": dest}, device_id_type=MESH)

    def x_recv(block, p):
        part = pl.ds(p * half, half)
        return pltpu.make_async_remote_copy(
            src_ref=act.at[partner, part], dst_ref=xbuf.at[block, part], send_sem=xs_sem.at[block, p],
            recv_sem=xr_sem.at[block, p], device_id={"seq": partner}, device_id_type=MESH)

    def extra_own(p):
        part = pl.ds(p * half, half)
        return pltpu.make_async_copy(act.at[far, part], xbuf.at[n, part], xr_sem.at[n, p])

    def extra_send(p):
        part = pl.ds(p * half, half)
        return pltpu.make_async_remote_copy(
            src_ref=act.at[far + 1, part], dst_ref=xbuf.at[n, part], send_sem=xs_sem.at[n, p], recv_sem=xr_sem.at[n, p],
            device_id={"seq": partner}, device_id_type=MESH)

    def y_send(slot):
        extra = slot // n
        seq = (1 - extra) * me + extra * (far + core)
        return pltpu.make_async_remote_copy(
            src_ref=ybuf.at[slot], dst_ref=out.at[seq], send_sem=ys_sem.at[slot], recv_sem=yr_sem.at[seq],
            device_id={"seq": slot - extra * n}, device_id_type=MESH)

    def y_recv(block):
        return pltpu.make_async_remote_copy(
            src_ref=ybuf.at[block], dst_ref=out.at[block], send_sem=ys_sem.at[block], recv_sem=yr_sem.at[block],
            device_id={"seq": block}, device_id_type=MESH)

    def y_own(slot):
        extra = slot // n
        seq = (1 - extra) * me + extra * (far + core)
        return pltpu.make_async_copy(ybuf.at[slot], out.at[seq], yr_sem.at[seq])

    vectors = [pltpu.make_async_copy(src, dst, vec_sem.at[k]) for k, (src, dst) in enumerate((
        (ln1s_hbm, ln1s), (ln1b_hbm, ln1b), (b_sp_hbm, b_sp), (b_in_hbm, b_in), (ln2s_hbm, ln2s), (ln2b_hbm, ln2b),
        (b_out_hbm, b_out)))]

    barrier = pltpu.get_barrier_semaphore()
    for k in range(1, n):
        pl.semaphore_signal(barrier, inc=1, device_id={"seq": lax.rem(me + k, n)}, device_id_type=MESH)
    for p in range(2):
        own_x(p).start()
    for copy in vectors:
        copy.start()
    for j in range(2 * gate_tiles):
        wi_copy((j + gate_tiles) % (2 * gate_tiles)).start()
    pl.semaphore_wait(barrier, n - 1)
    for dest in (far, partner, far + 1):
        for p in range(2):
            x_send(dest, p).start()
    @pl.when(me == 0)
    def _():
        for p in range(2):
            extra_send(p).start()
            extra_own(p).start()

    for j in range(length // LANES):
        ws_copy(j).start()
    mk_copy().start()
    for j in range(width // LANES):
        wo_copy(j).start()

    for copy in vectors:
        copy.wait()
    for i in range(n):
        at = pl.ds(i * rows, rows)
        bias[at, :] = jnp.broadcast_to(b_sp[:, at], (LANES, rows)).T

    def stage_a(t, first):
        if first:
            pieces = [(me, 0), (me, 1)]
            for p in range(2):
                own_x(p).wait()
        else:
            near, extra = 1 - (t + 2) // 4, t // 4
            remote = 1 - near - extra
            side = t - 2
            pieces = [
                (near * partner + remote * (far + even0 * side) + extra * n, remote * (1 - even0) * side),
                (near * partner + remote * (far + even0 * side + (1 - even0)) + extra * n,
                 near + extra + remote * (even0 + (1 - even0) * side))]

            @pl.when(extra * (1 - core) == 1)
            def _():
                for p in range(2):
                    extra_own(p).wait()

            @pl.when(extra * (1 - core) == 0)
            def _():
                for block, p in pieces:
                    x_recv(block, p).wait_recv()

        starts = [pl.multiple_of(block * rows + p * half, half) for block, p in pieces]
        step1 = 64
        for k, (block, p) in enumerate(pieces):
            for r in range(half // step1):
                x = xbuf[block, pl.ds(pl.multiple_of(p * half, half) + r * step1, step1), :].astype(F32)
                x = layer_norm(x, ln1s[...], ln1b[...]).astype(BF16)
                for j in range(width // LANES):
                    u[j, pl.ds(k * half + r * step1, step1), :] = x[:, j * LANES:(j + 1) * LANES]

        def chunk(c):
            tiles = range(c * per, (c + 1) * per)
            acc = jnp.dot(wide(u, range(width // LANES)), wide(wi, tiles), preferred_element_type=F32)
            return gelu(acc + b_in[:, pl.ds(c * COLS, COLS)]).astype(BF16), jnp.minimum(jnp.abs(acc[:, :LANES]), 0.0)

        def put(dst, c, value):
            for j in range(per):
                for k in range(2):
                    dst[c * per + j, pl.ds(starts[k], half), :] = value[k * half:(k + 1) * half, j * LANES:(j + 1) * LANES]

        early = 2
        for c in range(n_cols):
            if first and c in (0, early):
                for j in range(c * per, (early if c == 0 else n_cols) * per):
                    wi_copy(gate_tiles + j).wait()
            value, _ = chunk(n_cols + c)
            put(vn, c, value)
            value = value.astype(F32)
            tiles = [value[:, j * LANES:(j + 1) * LANES] for j in range(per)]
            if c == 0:
                pivot = tiles[0]
                stat[0] = pivot
                tiles = tiles[1:]
            else:
                pivot = stat[0]
            diffs = [v - pivot for v in tiles]
            total = sum(diffs[1:], diffs[0])
            squares = sum([d * d for d in diffs[1:]], diffs[0] * diffs[0])
            stat[1] = total if c == 0 else stat[1] + total
            stat[2] = squares if c == 0 else stat[2] + squares
        if first:
            for j in range(gate_tiles):
                wi_copy(j).wait()
        total = stat[1]
        mean_lane = stat[0] + total * (1.0 / gate_tiles)
        mean = jnp.sum(mean_lane, axis=-1, keepdims=True) * (1.0 / LANES)
        away = mean_lane - mean
        spread = (stat[2] - total * total * (1.0 / gate_tiles)) + gate_tiles * (away * away)
        var = jnp.maximum(jnp.sum(spread, axis=-1, keepdims=True) * (1.0 / gate), 0.0)
        stat[0] = jnp.broadcast_to(mean, (rows, LANES))
        stat[1] = jnp.broadcast_to(lax.rsqrt(var + LN_EPS), (rows, LANES))

        def norm(j, mean_now):
            for k in range(2):
                part = pl.ds(starts[k], half)
                here = pl.ds(k * half, half)
                value = (vn[j, part, :].astype(F32) - mean_now[k * half:(k + 1) * half]) * stat[1, here]
                vn[j, part, :] = (value * ln2s[:, lanes(j)] + ln2b[:, lanes(j)]).astype(BF16)

        for c in range(n_cols):
            value, zero = chunk(c)
            put(g, c, value)
            mean_now = stat[0] + zero
            for j in range(c * per, (c + 1) * per):
                norm(j, mean_now)

    def stage_b(slot, i):
        at = pl.ds(i * rows, rows)
        depth = (i + 1) * rows
        base = pl.multiple_of(slot // n * length, rows) if i == 0 else 0
        for j in range(depth // LANES):
            ws[j, at, :] = jnp.where(mk[at, lanes(j)] > 0, ws[j, at, :].astype(F32), 0.0).astype(BF16)
        for c in range(n_cols):
            tiles = range(c * per, (c + 1) * per)
            s = jnp.dot(wide(ws, range(depth // LANES), at), wide(vn, tiles, pl.ds(base, depth)), preferred_element_type=F32)
            for j in range(per):
                t = (s[:, j * LANES:(j + 1) * LANES] + bias[at, :]).astype(BF16).astype(F32)
                q[tiles[j]] = (g[tiles[j], pl.ds(base + i * rows, rows), :].astype(F32) * t).astype(BF16)
        for c in range(width // COLS):
            cols = pl.ds(c * COLS, COLS)
            y = jnp.dot(wide(q, range(gate_tiles)), wide(wo, range(c * per, (c + 1) * per)), preferred_element_type=F32)
            ybuf[slot, :, cols] = (xbuf[slot, :, cols].astype(F32) + (y + b_out[:, cols])).astype(BF16)

    stage_a(0, True)

    def outer(k, carry):
        last = k // n
        def upto(k):
            return (even0 * (3 + (k + 3) // 4 + k // 4) + odd0 * (2 + (k + 2) // 4 + 2 * ((k + 1) // 4)) + chip * n)

        def one(p, c):
            late = (p + 1) // 4
            stage_a(p + odd0 * (2 * ((p + 2) // 4 - late) - late), False)
            return c

        lax.fori_loop(jnp.where(k == 0, 1, upto(k - 1)), upto(k), one, 0)

        @pl.when(k == 0)
        def _():
            for j in range(length // LANES):
                ws_copy(j).wait()
            mk_copy().wait()
            for j in range(width // LANES):
                wo_copy(j).wait()

        slot = (even0 * ((1 - last) * lax.rem(k + 2, n) + last * n) + odd0 * (k + (k + 2) // 4 * (n + 2 - 2 * k))
                + chip * (k + 1))
        block = lax.rem(slot, n)
        for i in range(n):
            pl.when(block == i)(functools.partial(stage_b, slot, i))

        @pl.when(me == block)
        def _():
            y_own(slot).start()

        @pl.when(me != block)
        def _():
            y_send(slot).start()

        return carry

    lax.fori_loop(0, (1 - chip) * (n + 1) + chip * (n - 1), outer, 0)

    for k in range(1, n):
        for p in range(2):
            x_send(lax.rem(me + k, n), p).wait_send()

    @pl.when(me == 0)
    def _():
        for p in range(2):
            extra_send(p).wait_send()
        y_own(n).wait()

    @pl.when(me == 1)
    def _():
        y_send(n).wait_send()

    @pl.when((me != 0) & (chip == 0))
    def _():
        y_send(0).wait_send()

    for block in range(1, n):
        @pl.when(me != block)
        def _():
            y_send(block).wait_send()

    for seq in range(n):
        @pl.when((me != seq) & ((me != 0) | (seq != 2)))
        def _():
            y_recv(seq).wait_recv()

    y_own(me).wait()


def solution(mesh):
    n = mesh.shape["seq"]
    row_spec = P("data", "seq", None)

    def local_block(act_in, ln1_scale, ln1_bias, w_in, b_in, ln2_scale, ln2_bias, w_spatial, b_spatial, causal_mask, w_out, b_out):
        rows, width = act_in.shape[1:]
        length = n * rows
        gate = w_out.shape[0]
        hbm = pl.BlockSpec(memory_space=pl.ANY)

        def row(v):
            return v.reshape(1, -1)

        return pl.pallas_call(
            functools.partial(body, n),
            out_shape=pltpu.VMEM(act_in.shape, act_in.dtype),
            in_specs=[hbm] * 12,
            out_specs=hbm,
            scratch_shapes=[
                pltpu.VMEM((1, width), F32),
                pltpu.VMEM((1, width), F32),
                pltpu.VMEM((1, 2 * gate), F32),
                pltpu.VMEM((1, gate), F32),
                pltpu.VMEM((1, gate), F32),
                pltpu.VMEM((1, length), F32),
                pltpu.VMEM((1, width), F32),
                pltpu.VMEM((n + 1, rows, width), BF16),
                pltpu.VMEM((2 * gate // LANES, width, LANES), BF16),
                pltpu.VMEM((width // LANES, gate, LANES), BF16),
                pltpu.VMEM((length // LANES, length, LANES), BF16),
                pltpu.VMEM((length, length), jnp.int32),
                pltpu.VMEM((gate // LANES, length + rows, LANES), BF16),
                pltpu.VMEM((gate // LANES, length + rows, LANES), BF16),
                pltpu.VMEM((width // LANES, rows, LANES), BF16),
                pltpu.VMEM((gate // LANES, rows, LANES), BF16),
                pltpu.VMEM((n + 1, rows, width), BF16),
                pltpu.VMEM((length, LANES), F32),
                pltpu.VMEM((3, rows, LANES), F32),
                pltpu.SemaphoreType.DMA((n + 1, 2)),
                pltpu.SemaphoreType.DMA((n + 1, 2)),
                pltpu.SemaphoreType.DMA((n + 1,)),
                pltpu.SemaphoreType.DMA((n,)),
                pltpu.SemaphoreType.DMA((2 * gate // LANES,)),
                pltpu.SemaphoreType.DMA((width // LANES,)),
                pltpu.SemaphoreType.DMA((length // LANES,)),
                pltpu.SemaphoreType.DMA,
                pltpu.SemaphoreType.DMA((7,)),
            ],
            compiler_params=pltpu.CompilerParams(
                collective_id=0, has_side_effects=True, vmem_limit_bytes=60 * 1024 * 1024),
            name="gmlp",
        )(act_in, row(ln1_scale), row(ln1_bias), w_in, row(b_in), row(ln2_scale), row(ln2_bias),
          w_spatial, row(b_spatial), causal_mask, w_out, row(b_out))

    return jax.shard_map(local_block, mesh=mesh, in_specs=(row_spec,) + (P(),) * 11, out_specs=row_spec, check_vma=False)
```

```python
import functools

import jax
import jax.numpy as jnp
from jax import lax
from jax.experimental import pallas as pl
from jax.experimental.pallas import tpu as pltpu
from jax.sharding import PartitionSpec as P

LN_EPS = 1e-6
GELU_A = 0.7978845608028654
GELU_B = GELU_A * 0.044715
COLS = 512
LANES = 128
MESH = pl.DeviceIdType.MESH
F32 = jnp.float32
BF16 = jnp.bfloat16


def gelu(a):
    return a * jax.nn.sigmoid(a * (2 * GELU_A + 2 * GELU_B * (a * a)))


def layer_norm(x, gain, shift):
    width = x.shape[-1]
    mean = jnp.sum(x, axis=-1, keepdims=True) * (1.0 / width)
    centered = x - mean
    var = jnp.sum(centered * centered, axis=-1, keepdims=True) * (1.0 / width)
    return centered * lax.rsqrt(var + LN_EPS) * gain + shift


def wide(ref, tiles, *where):
    return jnp.concatenate([ref[(j, *where)] for j in tiles], axis=1)


def body(n, act, ln1s_hbm, ln1b_hbm, w_in, b_in_hbm, ln2s_hbm, ln2b_hbm, w_sp, b_sp_hbm, mask, w_out, b_out_hbm, out,
         ln1s, ln1b, b_in, ln2s, ln2b, b_sp, b_out, xbuf, wi, wo, ws, mk, vn, g, u, q, ybuf, bias, stat,
         xs_sem, xr_sem, ys_sem, yr_sem, wi_sem, wo_sem, ws_sem, mk_sem, vec_sem):
    me = lax.axis_index("seq")
    chip, core = me // 2, lax.rem(me, 2)
    partner = chip * 2 + 1 - core
    far = (1 - chip) * 2
    even0 = (1 - chip) * (1 - core)
    odd0 = (1 - chip) * core
    rows, width = act.shape[1], act.shape[2]
    length = n * rows
    half = rows // 2
    gate = w_out.shape[0]
    gate_tiles = gate // LANES
    n_cols = gate // COLS
    per = COLS // LANES

    def lanes(j):
        return pl.ds(j * LANES, LANES)

    def wi_copy(j):
        return pltpu.make_async_copy(w_in.at[:, lanes(j)], wi.at[j], wi_sem.at[j])

    def ws_copy(j):
        return pltpu.make_async_copy(w_sp.at[:, lanes(j)], ws.at[j], ws_sem.at[j])

    def wo_copy(j):
        return pltpu.make_async_copy(w_out.at[:, lanes(j)], wo.at[j], wo_sem.at[j])

    def mk_copy():
        return pltpu.make_async_copy(mask, mk, mk_sem)

    def own_x(p):
        part = pl.ds(p * half, half)
        return pltpu.make_async_copy(act.at[me, part], xbuf.at[me, part], xr_sem.at[me, p])

    def x_send(dest, p):
        part = pl.ds(p * half, half)
        return pltpu.make_async_remote_copy(
            src_ref=act.at[dest, part], dst_ref=xbuf.at[me, part], send_sem=xs_sem.at[dest, p], recv_sem=xr_sem.at[me, p],
            device_id={"seq": dest}, device_id_type=MESH)

    def x_recv(block, p):
        part = pl.ds(p * half, half)
        return pltpu.make_async_remote_copy(
            src_ref=act.at[partner, part], dst_ref=xbuf.at[block, part], send_sem=xs_sem.at[block, p],
            recv_sem=xr_sem.at[block, p], device_id={"seq": partner}, device_id_type=MESH)

    def extra_own(p):
        part = pl.ds(p * half, half)
        return pltpu.make_async_copy(act.at[far, part], xbuf.at[n, part], xr_sem.at[n, p])

    def y_send(block):
        return pltpu.make_async_remote_copy(
            src_ref=ybuf.at[block], dst_ref=out.at[me], send_sem=ys_sem.at[block], recv_sem=yr_sem.at[me],
            device_id={"seq": block}, device_id_type=MESH)

    def y_recv(block):
        return pltpu.make_async_remote_copy(
            src_ref=ybuf.at[block], dst_ref=out.at[block], send_sem=ys_sem.at[block], recv_sem=yr_sem.at[block],
            device_id={"seq": block}, device_id_type=MESH)

    def y_own(slot):
        extra = slot // n
        seq = (1 - extra) * me + extra * far
        return pltpu.make_async_copy(ybuf.at[slot], out.at[seq], yr_sem.at[seq])

    vectors = [pltpu.make_async_copy(src, dst, vec_sem.at[k]) for k, (src, dst) in enumerate((
        (ln1s_hbm, ln1s), (ln1b_hbm, ln1b), (b_sp_hbm, b_sp), (b_in_hbm, b_in), (ln2s_hbm, ln2s), (ln2b_hbm, ln2b),
        (b_out_hbm, b_out)))]

    barrier = pltpu.get_barrier_semaphore()
    for k in range(1, n):
        pl.semaphore_signal(barrier, inc=1, device_id={"seq": lax.rem(me + k, n)}, device_id_type=MESH)
    for p in range(2):
        own_x(p).start()
    for copy in vectors:
        copy.start()
    for j in range(2 * gate_tiles):
        wi_copy((j + gate_tiles) % (2 * gate_tiles)).start()
    pl.semaphore_wait(barrier, n - 1)
    for dest in (far, partner, far + 1):
        for p in range(2):
            x_send(dest, p).start()
    @pl.when(me == 0)
    def _():
        for p in range(2):
            extra_own(p).start()

    for j in range(length // LANES):
        ws_copy(j).start()
    mk_copy().start()
    for j in range(width // LANES):
        wo_copy(j).start()

    for copy in vectors:
        copy.wait()
    for i in range(n):
        at = pl.ds(i * rows, rows)
        bias[at, :] = jnp.broadcast_to(b_sp[:, at], (LANES, rows)).T

    def stage_a(t, first):
        if first:
            pieces = [(me, 0), (me, 1)]
            for p in range(2):
                own_x(p).wait()
        else:
            near, extra = 1 - (t + 2) // 4, t // 4
            remote = 1 - near - extra
            side = t - 2
            pieces = [
                (near * partner + remote * (far + even0 * side) + extra * n, remote * (1 - even0) * side),
                (near * partner + remote * (far + even0 * side + (1 - even0)) + extra * n,
                 near + extra + remote * (even0 + (1 - even0) * side))]

            @pl.when(extra == 1)
            def _():
                for p in range(2):
                    extra_own(p).wait()

            @pl.when(extra == 0)
            def _():
                for block, p in pieces:
                    x_recv(block, p).wait_recv()

        starts = [pl.multiple_of(lax.rem(block, n) * rows + p * half, half) for block, p in pieces]
        step1 = 64
        for k, (block, p) in enumerate(pieces):
            for r in range(half // step1):
                x = xbuf[block, pl.ds(pl.multiple_of(p * half, half) + r * step1, step1), :].astype(F32)
                x = layer_norm(x, ln1s[...], ln1b[...]).astype(BF16)
                for j in range(width // LANES):
                    u[j, pl.ds(k * half + r * step1, step1), :] = x[:, j * LANES:(j + 1) * LANES]

        def chunk(c):
            tiles = range(c * per, (c + 1) * per)
            acc = jnp.dot(wide(u, range(width // LANES)), wide(wi, tiles), preferred_element_type=F32)
            return gelu(acc + b_in[:, pl.ds(c * COLS, COLS)]).astype(BF16), jnp.minimum(jnp.abs(acc[:, :LANES]), 0.0)

        def put(dst, c, value):
            for j in range(per):
                for k in range(2):
                    dst[c * per + j, pl.ds(starts[k], half), :] = value[k * half:(k + 1) * half, j * LANES:(j + 1) * LANES]

        early = 2
        for c in range(n_cols):
            if first and c in (0, early):
                for j in range(c * per, (early if c == 0 else n_cols) * per):
                    wi_copy(gate_tiles + j).wait()
            value, _ = chunk(n_cols + c)
            put(vn, c, value)
            value = value.astype(F32)
            tiles = [value[:, j * LANES:(j + 1) * LANES] for j in range(per)]
            if c == 0:
                pivot = tiles[0]
                stat[0] = pivot
                tiles = tiles[1:]
            else:
                pivot = stat[0]
            diffs = [v - pivot for v in tiles]
            total = sum(diffs[1:], diffs[0])
            squares = sum([d * d for d in diffs[1:]], diffs[0] * diffs[0])
            stat[1] = total if c == 0 else stat[1] + total
            stat[2] = squares if c == 0 else stat[2] + squares
        if first:
            for j in range(gate_tiles):
                wi_copy(j).wait()
        total = stat[1]
        mean_lane = stat[0] + total * (1.0 / gate_tiles)
        mean = jnp.sum(mean_lane, axis=-1, keepdims=True) * (1.0 / LANES)
        away = mean_lane - mean
        spread = (stat[2] - total * total * (1.0 / gate_tiles)) + gate_tiles * (away * away)
        var = jnp.maximum(jnp.sum(spread, axis=-1, keepdims=True) * (1.0 / gate), 0.0)
        stat[0] = jnp.broadcast_to(mean, (rows, LANES))
        stat[1] = jnp.broadcast_to(lax.rsqrt(var + LN_EPS), (rows, LANES))

        def norm(j, mean_now):
            for k in range(2):
                part = pl.ds(starts[k], half)
                here = pl.ds(k * half, half)
                value = (vn[j, part, :].astype(F32) - mean_now[k * half:(k + 1) * half]) * stat[1, here]
                vn[j, part, :] = (value * ln2s[:, lanes(j)] + ln2b[:, lanes(j)]).astype(BF16)

        for c in range(n_cols):
            value, zero = chunk(c)
            put(g, c, value)
            mean_now = stat[0] + zero
            for j in range(c * per, (c + 1) * per):
                norm(j, mean_now)

    def stage_b(slot, i):
        at = pl.ds(i * rows, rows)
        depth = (i + 1) * rows
        for j in range(depth // LANES):
            ws[j, at, :] = jnp.where(mk[at, lanes(j)] > 0, ws[j, at, :].astype(F32), 0.0).astype(BF16)
        for c in range(n_cols):
            tiles = range(c * per, (c + 1) * per)
            s = jnp.dot(wide(ws, range(depth // LANES), at), wide(vn, tiles, pl.ds(0, depth)), preferred_element_type=F32)
            for j in range(per):
                t = (s[:, j * LANES:(j + 1) * LANES] + bias[at, :]).astype(BF16).astype(F32)
                q[tiles[j]] = (g[tiles[j], at, :].astype(F32) * t).astype(BF16)
        for c in range(width // COLS):
            cols = pl.ds(c * COLS, COLS)
            y = jnp.dot(wide(q, range(gate_tiles)), wide(wo, range(c * per, (c + 1) * per)), preferred_element_type=F32)
            ybuf[slot, :, cols] = (xbuf[slot, :, cols].astype(F32) + (y + b_out[:, cols])).astype(BF16)

    stage_a(0, True)

    def outer(k, carry):
        last = k // n
        def upto(k):
            return even0 * (3 + (k + 3) // 4 + k // 4) + odd0 * (2 + 2 * ((k + 2) // 4)) + chip * n

        def one(t, c):
            stage_a(t, False)
            return c

        lax.fori_loop(jnp.where(k == 0, 1, upto(k - 1)), upto(k), one, 0)

        @pl.when(k == 0)
        def _():
            for j in range(length // LANES):
                ws_copy(j).wait()
            mk_copy().wait()
            for j in range(width // LANES):
                wo_copy(j).wait()

        slot = (even0 * ((1 - last) * lax.rem(k + 2, n) + last * n)
                + odd0 * (k + (k + 2) // 4 * (n + 1 - 2 * k))
                + chip * (1 - core) * (k + 1)
                + chip * core * (1 - k + (k + 2) // 4 * (2 * k - 1)))
        block = lax.rem(slot, n)
        for i in range(n):
            pl.when(block == i)(functools.partial(stage_b, slot, i))

        @pl.when(me == block)
        def _():
            y_own(slot).start()

        @pl.when(me != block)
        def _():
            y_send(block).start()

        return carry

    lax.fori_loop(0, n + (1 - core) * (1 - 2 * chip), outer, 0)

    for k in range(1, n):
        for p in range(2):
            x_send(lax.rem(me + k, n), p).wait_send()

    @pl.when(me == 0)
    def _():
        y_own(n).wait()

    @pl.when(core == 1)
    def _():
        y_send(0).wait_send()

    for block in range(1, n):
        @pl.when(me != block)
        def _():
            y_send(block).wait_send()

    for seq in range(n):
        @pl.when((me != seq) & ((me != 0) | (seq != 2)))
        def _():
            y_recv(seq).wait_recv()

    y_own(me).wait()


def solution(mesh):
    n = mesh.shape["seq"]
    row_spec = P("data", "seq", None)

    def local_block(act_in, ln1_scale, ln1_bias, w_in, b_in, ln2_scale, ln2_bias, w_spatial, b_spatial, causal_mask, w_out, b_out):
        rows, width = act_in.shape[1:]
        length = n * rows
        gate = w_out.shape[0]
        hbm = pl.BlockSpec(memory_space=pl.ANY)

        def row(v):
            return v.reshape(1, -1)

        return pl.pallas_call(
            functools.partial(body, n),
            out_shape=pltpu.VMEM(act_in.shape, act_in.dtype),
            in_specs=[hbm] * 12,
            out_specs=hbm,
            scratch_shapes=[
                pltpu.VMEM((1, width), F32),
                pltpu.VMEM((1, width), F32),
                pltpu.VMEM((1, 2 * gate), F32),
                pltpu.VMEM((1, gate), F32),
                pltpu.VMEM((1, gate), F32),
                pltpu.VMEM((1, length), F32),
                pltpu.VMEM((1, width), F32),
                pltpu.VMEM((n + 1, rows, width), BF16),
                pltpu.VMEM((2 * gate // LANES, width, LANES), BF16),
                pltpu.VMEM((width // LANES, gate, LANES), BF16),
                pltpu.VMEM((length // LANES, length, LANES), BF16),
                pltpu.VMEM((length, length), jnp.int32),
                pltpu.VMEM((gate // LANES, length, LANES), BF16),
                pltpu.VMEM((gate // LANES, length, LANES), BF16),
                pltpu.VMEM((width // LANES, rows, LANES), BF16),
                pltpu.VMEM((gate // LANES, rows, LANES), BF16),
                pltpu.VMEM((n + 1, rows, width), BF16),
                pltpu.VMEM((length, LANES), F32),
                pltpu.VMEM((3, rows, LANES), F32),
                pltpu.SemaphoreType.DMA((n + 1, 2)),
                pltpu.SemaphoreType.DMA((n + 1, 2)),
                pltpu.SemaphoreType.DMA((n + 1,)),
                pltpu.SemaphoreType.DMA((n,)),
                pltpu.SemaphoreType.DMA((2 * gate // LANES,)),
                pltpu.SemaphoreType.DMA((width // LANES,)),
                pltpu.SemaphoreType.DMA((length // LANES,)),
                pltpu.SemaphoreType.DMA,
                pltpu.SemaphoreType.DMA((7,)),
            ],
            compiler_params=pltpu.CompilerParams(
                collective_id=0, has_side_effects=True, vmem_limit_bytes=60 * 1024 * 1024),
            name="gmlp",
        )(act_in, row(ln1_scale), row(ln1_bias), w_in, row(b_in), row(ln2_scale), row(ln2_bias),
          w_spatial, row(b_spatial), causal_mask, w_out, row(b_out))

    return jax.shard_map(local_block, mesh=mesh, in_specs=(row_spec,) + (P(),) * 11, out_specs=row_spec, check_vma=False)
```

```python
import functools

import jax
import jax.numpy as jnp
from jax import lax
from jax.experimental import pallas as pl
from jax.experimental.pallas import tpu as pltpu
from jax.sharding import PartitionSpec as P

LN_EPS = 1e-6
GELU_A = 0.7978845608028654
GELU_B = GELU_A * 0.044715
COLS = 512
LANES = 128
MESH = pl.DeviceIdType.MESH
F32 = jnp.float32
BF16 = jnp.bfloat16


def gelu(a):
    return a * jax.nn.sigmoid(a * (2 * GELU_A + 2 * GELU_B * (a * a)))


def layer_norm(x, gain, shift):
    width = x.shape[-1]
    mean = jnp.sum(x, axis=-1, keepdims=True) * (1.0 / width)
    centered = x - mean
    var = jnp.sum(centered * centered, axis=-1, keepdims=True) * (1.0 / width)
    return centered * lax.rsqrt(var + LN_EPS) * gain + shift


def wide(ref, tiles, *where):
    return jnp.concatenate([ref[(j, *where)] for j in tiles], axis=1)


def body(n, act, ln1s_hbm, ln1b_hbm, w_in, b_in_hbm, ln2s_hbm, ln2b_hbm, w_sp, b_sp_hbm, mask, w_out, b_out_hbm, out,
         ln1s, ln1b, b_in, ln2s, ln2b, b_sp, b_out, xbuf, wi, wo, ws, mk, vn, g, u, q, ybuf, bias, stat,
         xs_sem, xr_sem, ys_sem, yr_sem, wi_sem, wo_sem, ws_sem, mk_sem, vec_sem):
    me = lax.axis_index("seq")
    chip, core = me // 2, lax.rem(me, 2)
    partner = chip * 2 + 1 - core
    far = (1 - chip) * 2
    early0 = (1 - chip) * core
    late0 = (1 - chip) * (1 - core)
    rows, width = act.shape[1], act.shape[2]
    length = n * rows
    half = rows // 2
    gate = w_out.shape[0]
    gate_tiles = gate // LANES
    n_cols = gate // COLS
    per = COLS // LANES

    def lanes(j):
        return pl.ds(j * LANES, LANES)

    def wi_copy(j):
        return pltpu.make_async_copy(w_in.at[:, lanes(j)], wi.at[j], wi_sem.at[j])

    def ws_copy(j):
        return pltpu.make_async_copy(w_sp.at[:, lanes(j)], ws.at[j], ws_sem.at[j])

    def wo_copy(j):
        return pltpu.make_async_copy(w_out.at[:, lanes(j)], wo.at[j], wo_sem.at[j])

    def mk_copy():
        return pltpu.make_async_copy(mask, mk, mk_sem)

    def own_x(p):
        part = pl.ds(p * half, half)
        return pltpu.make_async_copy(act.at[me, part], xbuf.at[me, part], xr_sem.at[me, p])

    def x_send(dest, p):
        part = pl.ds(p * half, half)
        return pltpu.make_async_remote_copy(
            src_ref=act.at[dest, part], dst_ref=xbuf.at[me, part], send_sem=xs_sem.at[dest, p], recv_sem=xr_sem.at[me, p],
            device_id={"seq": dest}, device_id_type=MESH)

    def x_recv(block, p):
        part = pl.ds(p * half, half)
        return pltpu.make_async_remote_copy(
            src_ref=act.at[partner, part], dst_ref=xbuf.at[block, part], send_sem=xs_sem.at[block, p],
            recv_sem=xr_sem.at[block, p], device_id={"seq": partner}, device_id_type=MESH)

    def extra_own(p):
        part = pl.ds(p * half, half)
        return pltpu.make_async_copy(act.at[far, part], xbuf.at[n, part], xr_sem.at[n, p])

    def extra_send(p):
        part = pl.ds(p * half, half)
        return pltpu.make_async_remote_copy(
            src_ref=act.at[far + 1, part], dst_ref=xbuf.at[n, part], send_sem=xs_sem.at[n, p], recv_sem=xr_sem.at[n, p],
            device_id={"seq": partner}, device_id_type=MESH)

    def y_send(slot):
        extra = slot // n
        seq = (1 - extra) * me + extra * (far + core)
        return pltpu.make_async_remote_copy(
            src_ref=ybuf.at[slot], dst_ref=out.at[seq], send_sem=ys_sem.at[slot], recv_sem=yr_sem.at[seq],
            device_id={"seq": slot - extra * n}, device_id_type=MESH)

    def y_recv(block):
        return pltpu.make_async_remote_copy(
            src_ref=ybuf.at[block], dst_ref=out.at[block], send_sem=ys_sem.at[block], recv_sem=yr_sem.at[block],
            device_id={"seq": block}, device_id_type=MESH)

    def y_own(slot):
        extra = slot // n
        seq = (1 - extra) * me + extra * (far + core)
        return pltpu.make_async_copy(ybuf.at[slot], out.at[seq], yr_sem.at[seq])

    vectors = [pltpu.make_async_copy(src, dst, vec_sem.at[k]) for k, (src, dst) in enumerate((
        (ln1s_hbm, ln1s), (ln1b_hbm, ln1b), (b_sp_hbm, b_sp), (b_in_hbm, b_in), (ln2s_hbm, ln2s), (ln2b_hbm, ln2b),
        (b_out_hbm, b_out)))]

    barrier = pltpu.get_barrier_semaphore()
    for k in range(1, n):
        pl.semaphore_signal(barrier, inc=1, device_id={"seq": lax.rem(me + k, n)}, device_id_type=MESH)
    for p in range(2):
        own_x(p).start()
    for copy in vectors:
        copy.start()
    for j in range(2 * gate_tiles):
        wi_copy((j + gate_tiles) % (2 * gate_tiles)).start()
    pl.semaphore_wait(barrier, n - 1)
    for dest in (far + chip, partner, far + 1 - chip):
        for p in range(2):
            x_send(dest, p).start()
    @pl.when(me == 0)
    def _():
        for p in range(2):
            extra_send(p).start()
            extra_own(p).start()

    for j in range(length // LANES):
        ws_copy(j).start()
    mk_copy().start()
    for j in range(width // LANES):
        wo_copy(j).start()

    for copy in vectors:
        copy.wait()
    for i in range(n):
        at = pl.ds(i * rows, rows)
        bias[at, :] = jnp.broadcast_to(b_sp[:, at], (LANES, rows)).T

    def stage_a(t, first):
        if first:
            pieces = [(me, 0), (me, 1)]
            for p in range(2):
                own_x(p).wait()
        else:
            near, extra = 1 - (t + 2) // 4, t // 4
            remote = 1 - near - extra
            side = t - 2
            pieces = [
                (near * partner + remote * (far + early0 * side) + extra * n, remote * (1 - early0) * side),
                (near * partner + remote * (far + early0 * side + (1 - early0)) + extra * n,
                 near + extra + remote * (early0 + (1 - early0) * side))]

            @pl.when(extra * (1 - core) == 1)
            def _():
                for p in range(2):
                    extra_own(p).wait()

            @pl.when(extra * (1 - core) == 0)
            def _():
                for block, p in pieces:
                    x_recv(block, p).wait_recv()

        starts = [pl.multiple_of(lax.rem(block, n) * rows + p * half, half) for block, p in pieces]
        step1 = 64
        for k, (block, p) in enumerate(pieces):
            for r in range(half // step1):
                x = xbuf[block, pl.ds(pl.multiple_of(p * half, half) + r * step1, step1), :].astype(F32)
                x = layer_norm(x, ln1s[...], ln1b[...]).astype(BF16)
                for j in range(width // LANES):
                    u[j, pl.ds(k * half + r * step1, step1), :] = x[:, j * LANES:(j + 1) * LANES]

        def chunk(c):
            tiles = range(c * per, (c + 1) * per)
            acc = jnp.dot(wide(u, range(width // LANES)), wide(wi, tiles), preferred_element_type=F32)
            return gelu(acc + b_in[:, pl.ds(c * COLS, COLS)]).astype(BF16), jnp.minimum(jnp.abs(acc[:, :LANES]), 0.0)

        def put(dst, c, value):
            for j in range(per):
                for k in range(2):
                    dst[c * per + j, pl.ds(starts[k], half), :] = value[k * half:(k + 1) * half, j * LANES:(j + 1) * LANES]

        if first:
            for j in range(gate_tiles, 2 * gate_tiles):
                wi_copy(j).wait()
        for c in range(n_cols):
            value, _ = chunk(n_cols + c)
            put(vn, c, value)
            value = value.astype(F32)
            tiles = [value[:, j * LANES:(j + 1) * LANES] for j in range(per)]
            if c == 0:
                pivot = tiles[0]
                stat[0] = pivot
                tiles = tiles[1:]
            else:
                pivot = stat[0]
            diffs = [v - pivot for v in tiles]
            total = sum(diffs[1:], diffs[0])
            squares = sum([d * d for d in diffs[1:]], diffs[0] * diffs[0])
            stat[1] = total if c == 0 else stat[1] + total
            stat[2] = squares if c == 0 else stat[2] + squares
        if first:
            for j in range(gate_tiles):
                wi_copy(j).wait()
        total = stat[1]
        mean_lane = stat[0] + total * (1.0 / gate_tiles)
        mean = jnp.sum(mean_lane, axis=-1, keepdims=True) * (1.0 / LANES)
        away = mean_lane - mean
        spread = (stat[2] - total * total * (1.0 / gate_tiles)) + gate_tiles * (away * away)
        var = jnp.maximum(jnp.sum(spread, axis=-1, keepdims=True) * (1.0 / gate), 0.0)
        stat[0] = jnp.broadcast_to(mean, (rows, LANES))
        stat[1] = jnp.broadcast_to(lax.rsqrt(var + LN_EPS), (rows, LANES))

        def norm(j, mean_now):
            for k in range(2):
                part = pl.ds(starts[k], half)
                here = pl.ds(k * half, half)
                value = (vn[j, part, :].astype(F32) - mean_now[k * half:(k + 1) * half]) * stat[1, here]
                vn[j, part, :] = (value * ln2s[:, lanes(j)] + ln2b[:, lanes(j)]).astype(BF16)

        for c in range(n_cols):
            value, zero = chunk(c)
            put(g, c, value)
            mean_now = stat[0] + zero
            for j in range(c * per, (c + 1) * per):
                norm(j, mean_now)

    def stage_b(slot, i):
        at = pl.ds(i * rows, rows)
        depth = (i + 1) * rows
        for j in range(depth // LANES):
            ws[j, at, :] = jnp.where(mk[at, lanes(j)] > 0, ws[j, at, :].astype(F32), 0.0).astype(BF16)
        for c in range(n_cols):
            tiles = range(c * per, (c + 1) * per)
            s = jnp.dot(wide(ws, range(depth // LANES), at), wide(vn, tiles, pl.ds(0, depth)), preferred_element_type=F32)
            for j in range(per):
                t = (s[:, j * LANES:(j + 1) * LANES] + bias[at, :]).astype(BF16).astype(F32)
                q[tiles[j]] = (g[tiles[j], at, :].astype(F32) * t).astype(BF16)
        for c in range(width // COLS):
            cols = pl.ds(c * COLS, COLS)
            y = jnp.dot(wide(q, range(gate_tiles)), wide(wo, range(c * per, (c + 1) * per)), preferred_element_type=F32)
            ybuf[slot, :, cols] = (xbuf[slot, :, cols].astype(F32) + (y + b_out[:, cols])).astype(BF16)

    stage_a(0, True)

    def outer(k, carry):
        last = k // n
        def upto(k):
            return (early0 * (3 + (k + 3) // 4 + k // 4) + late0 * (2 + 2 * ((k + 2) // 4) + k // 4) + chip * n)

        def one(t, c):
            stage_a(t, False)
            return c

        lax.fori_loop(jnp.where(k == 0, 1, upto(k - 1)), upto(k), one, 0)

        @pl.when(k == 0)
        def _():
            for j in range(length // LANES):
                ws_copy(j).wait()
            mk_copy().wait()
            for j in range(width // LANES):
                wo_copy(j).wait()

        slot = early0 * ((1 - last) * lax.rem(k + 2, n) + last * n) + late0 * k + chip * (k + 1)
        block = lax.rem(slot, n)
        for i in range(n):
            pl.when(block == i)(functools.partial(stage_b, slot, i))

        @pl.when(me == block)
        def _():
            y_own(slot).start()

        @pl.when(me != block)
        def _():
            y_send(slot).start()

        return carry

    lax.fori_loop(0, (1 - chip) * (n + 1) + chip * (n - 1), outer, 0)

    for k in range(1, n):
        for p in range(2):
            x_send(lax.rem(me + k, n), p).wait_send()

    @pl.when(me == 0)
    def _():
        for p in range(2):
            extra_send(p).wait_send()
        y_own(n).wait()

    @pl.when(me == 1)
    def _():
        y_send(n).wait_send()

    @pl.when((me != 0) & (chip == 0))
    def _():
        y_send(0).wait_send()

    for block in range(1, n):
        @pl.when(me != block)
        def _():
            y_send(block).wait_send()

    for seq in range(n):
        @pl.when((me != seq) & ((me != 0) | (seq != 2)))
        def _():
            y_recv(seq).wait_recv()

    y_own(me).wait()


def solution(mesh):
    n = mesh.shape["seq"]
    row_spec = P("data", "seq", None)

    def local_block(act_in, ln1_scale, ln1_bias, w_in, b_in, ln2_scale, ln2_bias, w_spatial, b_spatial, causal_mask, w_out, b_out):
        rows, width = act_in.shape[1:]
        length = n * rows
        gate = w_out.shape[0]
        hbm = pl.BlockSpec(memory_space=pl.ANY)

        def row(v):
            return v.reshape(1, -1)

        return pl.pallas_call(
            functools.partial(body, n),
            out_shape=pltpu.VMEM(act_in.shape, act_in.dtype),
            in_specs=[hbm] * 12,
            out_specs=hbm,
            scratch_shapes=[
                pltpu.VMEM((1, width), F32),
                pltpu.VMEM((1, width), F32),
                pltpu.VMEM((1, 2 * gate), F32),
                pltpu.VMEM((1, gate), F32),
                pltpu.VMEM((1, gate), F32),
                pltpu.VMEM((1, length), F32),
                pltpu.VMEM((1, width), F32),
                pltpu.VMEM((n + 1, rows, width), BF16),
                pltpu.VMEM((2 * gate // LANES, width, LANES), BF16),
                pltpu.VMEM((width // LANES, gate, LANES), BF16),
                pltpu.VMEM((length // LANES, length, LANES), BF16),
                pltpu.VMEM((length, length), jnp.int32),
                pltpu.VMEM((gate // LANES, length, LANES), BF16),
                pltpu.VMEM((gate // LANES, length, LANES), BF16),
                pltpu.VMEM((width // LANES, rows, LANES), BF16),
                pltpu.VMEM((gate // LANES, rows, LANES), BF16),
                pltpu.VMEM((n + 1, rows, width), BF16),
                pltpu.VMEM((length, LANES), F32),
                pltpu.VMEM((3, rows, LANES), F32),
                pltpu.SemaphoreType.DMA((n + 1, 2)),
                pltpu.SemaphoreType.DMA((n + 1, 2)),
                pltpu.SemaphoreType.DMA((n + 1,)),
                pltpu.SemaphoreType.DMA((n,)),
                pltpu.SemaphoreType.DMA((2 * gate // LANES,)),
                pltpu.SemaphoreType.DMA((width // LANES,)),
                pltpu.SemaphoreType.DMA((length // LANES,)),
                pltpu.SemaphoreType.DMA,
                pltpu.SemaphoreType.DMA((7,)),
            ],
            compiler_params=pltpu.CompilerParams(
                collective_id=0, has_side_effects=True, vmem_limit_bytes=60 * 1024 * 1024),
            name="gmlp",
        )(act_in, row(ln1_scale), row(ln1_bias), w_in, row(b_in), row(ln2_scale), row(ln2_bias),
          w_spatial, row(b_spatial), causal_mask, w_out, row(b_out))

    return jax.shard_map(local_block, mesh=mesh, in_specs=(row_spec,) + (P(),) * 11, out_specs=row_spec, check_vma=False)
```

```python
import functools

import jax
import jax.numpy as jnp
from jax import lax
from jax.experimental import pallas as pl
from jax.experimental.pallas import tpu as pltpu
from jax.sharding import PartitionSpec as P

LN_EPS = 1e-6
GELU_A = 0.7978845608028654
GELU_B = GELU_A * 0.044715
COLS = 512
LANES = 128
MESH = pl.DeviceIdType.MESH
F32 = jnp.float32
BF16 = jnp.bfloat16


def gelu(a):
    return a * jax.nn.sigmoid(a * (2 * GELU_A + 2 * GELU_B * (a * a)))


def layer_norm(x, gain, shift):
    width = x.shape[-1]
    mean = jnp.sum(x, axis=-1, keepdims=True) * (1.0 / width)
    centered = x - mean
    var = jnp.sum(centered * centered, axis=-1, keepdims=True) * (1.0 / width)
    return centered * lax.rsqrt(var + LN_EPS) * gain + shift


def wide(ref, tiles, *where):
    return jnp.concatenate([ref[(j, *where)] for j in tiles], axis=1)


def body(n, act, ln1s_hbm, ln1b_hbm, w_in, b_in_hbm, ln2s_hbm, ln2b_hbm, w_sp, b_sp_hbm, mask, w_out, b_out_hbm, out,
         ln1s, ln1b, b_in, ln2s, ln2b, b_sp, b_out, xbuf, wi, wo, ws, mk, vn, g, u, q, ybuf, bias, stat,
         xs_sem, xr_sem, ys_sem, yr_sem, wi_sem, wo_sem, ws_sem, mk_sem, vec_sem):
    me = lax.axis_index("seq")
    chip, core = me // 2, lax.rem(me, 2)
    partner = chip * 2 + 1 - core
    far = (1 - chip) * 2
    early0 = (1 - chip) * core
    late0 = (1 - chip) * (1 - core)
    rows, width = act.shape[1], act.shape[2]
    length = n * rows
    half = rows // 2
    gate = w_out.shape[0]
    gate_tiles = gate // LANES
    n_cols = gate // COLS
    per = COLS // LANES

    def lanes(j):
        return pl.ds(j * LANES, LANES)

    def wi_copy(j):
        return pltpu.make_async_copy(w_in.at[:, lanes(j)], wi.at[j], wi_sem.at[j])

    def ws_copy(j):
        return pltpu.make_async_copy(w_sp.at[:, lanes(j)], ws.at[j], ws_sem.at[j])

    def wo_copy(j):
        return pltpu.make_async_copy(w_out.at[:, lanes(j)], wo.at[j], wo_sem.at[j])

    def mk_copy():
        return pltpu.make_async_copy(mask, mk, mk_sem)

    def own_x(p):
        part = pl.ds(p * half, half)
        return pltpu.make_async_copy(act.at[me, part], xbuf.at[me, part], xr_sem.at[me, p])

    def x_send(dest, p):
        part = pl.ds(p * half, half)
        return pltpu.make_async_remote_copy(
            src_ref=act.at[dest, part], dst_ref=xbuf.at[me, part], send_sem=xs_sem.at[dest, p], recv_sem=xr_sem.at[me, p],
            device_id={"seq": dest}, device_id_type=MESH)

    def x_recv(block, p):
        part = pl.ds(p * half, half)
        return pltpu.make_async_remote_copy(
            src_ref=act.at[partner, part], dst_ref=xbuf.at[block, part], send_sem=xs_sem.at[block, p],
            recv_sem=xr_sem.at[block, p], device_id={"seq": partner}, device_id_type=MESH)

    def extra_send(p):
        part = pl.ds(p * half, half)
        return pltpu.make_async_remote_copy(
            src_ref=act.at[far + 1, part], dst_ref=xbuf.at[n, part], send_sem=xs_sem.at[n, p], recv_sem=xr_sem.at[n, p],
            device_id={"seq": partner}, device_id_type=MESH)

    def y_send(slot):
        extra = slot // n
        seq = (1 - extra) * me + extra * (far + core)
        return pltpu.make_async_remote_copy(
            src_ref=ybuf.at[slot], dst_ref=out.at[seq], send_sem=ys_sem.at[slot], recv_sem=yr_sem.at[seq],
            device_id={"seq": slot - extra * n}, device_id_type=MESH)

    def y_recv(block):
        return pltpu.make_async_remote_copy(
            src_ref=ybuf.at[block], dst_ref=out.at[block], send_sem=ys_sem.at[block], recv_sem=yr_sem.at[block],
            device_id={"seq": block}, device_id_type=MESH)

    def y_own():
        return pltpu.make_async_copy(ybuf.at[me], out.at[me], yr_sem.at[me])

    vectors = [pltpu.make_async_copy(src, dst, vec_sem.at[k]) for k, (src, dst) in enumerate((
        (ln1s_hbm, ln1s), (ln1b_hbm, ln1b), (b_sp_hbm, b_sp), (b_in_hbm, b_in), (ln2s_hbm, ln2s), (ln2b_hbm, ln2b),
        (b_out_hbm, b_out)))]

    barrier = pltpu.get_barrier_semaphore()
    for k in range(1, n):
        pl.semaphore_signal(barrier, inc=1, device_id={"seq": lax.rem(me + k, n)}, device_id_type=MESH)
    for p in range(2):
        own_x(p).start()
    for copy in vectors:
        copy.start()
    for j in range(2 * gate_tiles):
        wi_copy((j + gate_tiles) % (2 * gate_tiles)).start()
    pl.semaphore_wait(barrier, n - 1)
    for dest in (far + chip, partner, far + 1 - chip):
        for p in range(2):
            x_send(dest, p).start()
    @pl.when(me == 0)
    def _():
        for p in range(2):
            extra_send(p).start()

    for j in range(length // LANES):
        ws_copy(j).start()
    mk_copy().start()
    for j in range(width // LANES):
        wo_copy(j).start()

    for copy in vectors:
        copy.wait()
    for i in range(n):
        at = pl.ds(i * rows, rows)
        bias[at, :] = jnp.broadcast_to(b_sp[:, at], (LANES, rows)).T

    def stage_a(t, first):
        if first:
            pieces = [(me, 0), (me, 1)]
            for p in range(2):
                own_x(p).wait()
        else:
            near, extra = 1 - (t + 2) // 4, t // 4
            remote = 1 - near - extra
            side = t - 2
            pieces = [
                (near * partner + remote * (far + early0 * side) + extra * n, remote * (1 - early0) * side),
                (near * partner + remote * (far + early0 * side + (1 - early0)) + extra * n,
                 near + extra + remote * (early0 + (1 - early0) * side))]

            for block, p in pieces:
                x_recv(block, p).wait_recv()
        starts = [pl.multiple_of(lax.rem(block, n) * rows + p * half, half) for block, p in pieces]
        step1 = 64
        for k, (block, p) in enumerate(pieces):
            for r in range(half // step1):
                x = xbuf[block, pl.ds(pl.multiple_of(p * half, half) + r * step1, step1), :].astype(F32)
                x = layer_norm(x, ln1s[...], ln1b[...]).astype(BF16)
                for j in range(width // LANES):
                    u[j, pl.ds(k * half + r * step1, step1), :] = x[:, j * LANES:(j + 1) * LANES]

        def chunk(c):
            tiles = range(c * per, (c + 1) * per)
            acc = jnp.dot(wide(u, range(width // LANES)), wide(wi, tiles), preferred_element_type=F32)
            return gelu(acc + b_in[:, pl.ds(c * COLS, COLS)]).astype(BF16), jnp.minimum(jnp.abs(acc[:, :LANES]), 0.0)

        def put(dst, c, value):
            for j in range(per):
                for k in range(2):
                    dst[c * per + j, pl.ds(starts[k], half), :] = value[k * half:(k + 1) * half, j * LANES:(j + 1) * LANES]

        if first:
            for j in range(gate_tiles, 2 * gate_tiles):
                wi_copy(j).wait()
        for c in range(n_cols):
            value, _ = chunk(n_cols + c)
            put(vn, c, value)
            value = value.astype(F32)
            tiles = [value[:, j * LANES:(j + 1) * LANES] for j in range(per)]
            if c == 0:
                pivot = tiles[0]
                stat[0] = pivot
                tiles = tiles[1:]
            else:
                pivot = stat[0]
            diffs = [v - pivot for v in tiles]
            total = sum(diffs[1:], diffs[0])
            squares = sum([d * d for d in diffs[1:]], diffs[0] * diffs[0])
            stat[1] = total if c == 0 else stat[1] + total
            stat[2] = squares if c == 0 else stat[2] + squares
        if first:
            for j in range(gate_tiles):
                wi_copy(j).wait()
        total = stat[1]
        mean_lane = stat[0] + total * (1.0 / gate_tiles)
        mean = jnp.sum(mean_lane, axis=-1, keepdims=True) * (1.0 / LANES)
        away = mean_lane - mean
        spread = (stat[2] - total * total * (1.0 / gate_tiles)) + gate_tiles * (away * away)
        var = jnp.maximum(jnp.sum(spread, axis=-1, keepdims=True) * (1.0 / gate), 0.0)
        stat[0] = jnp.broadcast_to(mean, (rows, LANES))
        stat[1] = jnp.broadcast_to(lax.rsqrt(var + LN_EPS), (rows, LANES))

        def norm(j, mean_now):
            for k in range(2):
                part = pl.ds(starts[k], half)
                here = pl.ds(k * half, half)
                value = (vn[j, part, :].astype(F32) - mean_now[k * half:(k + 1) * half]) * stat[1, here]
                vn[j, part, :] = (value * ln2s[:, lanes(j)] + ln2b[:, lanes(j)]).astype(BF16)

        for c in range(n_cols):
            value, zero = chunk(c)
            put(g, c, value)
            mean_now = stat[0] + zero
            for j in range(c * per, (c + 1) * per):
                norm(j, mean_now)

    def stage_b(slot, i):
        at = pl.ds(i * rows, rows)
        depth = (i + 1) * rows
        for j in range(depth // LANES):
            ws[j, at, :] = jnp.where(mk[at, lanes(j)] > 0, ws[j, at, :].astype(F32), 0.0).astype(BF16)
        for c in range(n_cols):
            tiles = range(c * per, (c + 1) * per)
            s = jnp.dot(wide(ws, range(depth // LANES), at), wide(vn, tiles, pl.ds(0, depth)), preferred_element_type=F32)
            for j in range(per):
                t = (s[:, j * LANES:(j + 1) * LANES] + bias[at, :]).astype(BF16).astype(F32)
                q[tiles[j]] = (g[tiles[j], at, :].astype(F32) * t).astype(BF16)
        for c in range(width // COLS):
            cols = pl.ds(c * COLS, COLS)
            y = jnp.dot(wide(q, range(gate_tiles)), wide(wo, range(c * per, (c + 1) * per)), preferred_element_type=F32)
            ybuf[slot, :, cols] = (xbuf[slot, :, cols].astype(F32) + (y + b_out[:, cols])).astype(BF16)

    stage_a(0, True)

    def outer(k, carry):
        last = k // n
        def upto(k):
            return (early0 * (3 + (k + 3) // 4 + k // 4) + late0 * (2 + 2 * ((k + 2) // 4)) + chip * n)

        def one(t, c):
            stage_a(t, False)
            return c

        lax.fori_loop(jnp.where(k == 0, 1, upto(k - 1)), upto(k), one, 0)

        @pl.when(k == 0)
        def _():
            for j in range(length // LANES):
                ws_copy(j).wait()
            mk_copy().wait()
            for j in range(width // LANES):
                wo_copy(j).wait()

        slot = early0 * ((1 - last) * lax.rem(k + 2, n) + last * n) + late0 * k + chip * (k + core)
        block = lax.rem(slot, n)
        for i in range(n):
            pl.when(block == i)(functools.partial(stage_b, slot, i))

        @pl.when(me == block)
        def _():
            y_own().start()

        @pl.when(me != block)
        def _():
            y_send(slot).start()

        return carry

    lax.fori_loop(0, n + core * (1 - 2 * chip), outer, 0)

    for k in range(1, n):
        for p in range(2):
            x_send(lax.rem(me + k, n), p).wait_send()

    @pl.when(me == 0)
    def _():
        for p in range(2):
            extra_send(p).wait_send()

    @pl.when(me == 1)
    def _():
        y_send(n).wait_send()

    @pl.when((me == 1) | (me == 2))
    def _():
        y_send(0).wait_send()

    for block in range(1, n):
        @pl.when(me != block)
        def _():
            y_send(block).wait_send()

    for seq in range(n):
        @pl.when(me != seq)
        def _():
            y_recv(seq).wait_recv()

    y_own().wait()


def solution(mesh):
    n = mesh.shape["seq"]
    row_spec = P("data", "seq", None)

    def local_block(act_in, ln1_scale, ln1_bias, w_in, b_in, ln2_scale, ln2_bias, w_spatial, b_spatial, causal_mask, w_out, b_out):
        rows, width = act_in.shape[1:]
        length = n * rows
        gate = w_out.shape[0]
        hbm = pl.BlockSpec(memory_space=pl.ANY)

        def row(v):
            return v.reshape(1, -1)

        return pl.pallas_call(
            functools.partial(body, n),
            out_shape=pltpu.VMEM(act_in.shape, act_in.dtype),
            in_specs=[hbm] * 12,
            out_specs=hbm,
            scratch_shapes=[
                pltpu.VMEM((1, width), F32),
                pltpu.VMEM((1, width), F32),
                pltpu.VMEM((1, 2 * gate), F32),
                pltpu.VMEM((1, gate), F32),
                pltpu.VMEM((1, gate), F32),
                pltpu.VMEM((1, length), F32),
                pltpu.VMEM((1, width), F32),
                pltpu.VMEM((n + 1, rows, width), BF16),
                pltpu.VMEM((2 * gate // LANES, width, LANES), BF16),
                pltpu.VMEM((width // LANES, gate, LANES), BF16),
                pltpu.VMEM((length // LANES, length, LANES), BF16),
                pltpu.VMEM((length, length), jnp.int32),
                pltpu.VMEM((gate // LANES, length, LANES), BF16),
                pltpu.VMEM((gate // LANES, length, LANES), BF16),
                pltpu.VMEM((width // LANES, rows, LANES), BF16),
                pltpu.VMEM((gate // LANES, rows, LANES), BF16),
                pltpu.VMEM((n + 1, rows, width), BF16),
                pltpu.VMEM((length, LANES), F32),
                pltpu.VMEM((3, rows, LANES), F32),
                pltpu.SemaphoreType.DMA((n + 1, 2)),
                pltpu.SemaphoreType.DMA((n + 1, 2)),
                pltpu.SemaphoreType.DMA((n + 1,)),
                pltpu.SemaphoreType.DMA((n,)),
                pltpu.SemaphoreType.DMA((2 * gate // LANES,)),
                pltpu.SemaphoreType.DMA((width // LANES,)),
                pltpu.SemaphoreType.DMA((length // LANES,)),
                pltpu.SemaphoreType.DMA,
                pltpu.SemaphoreType.DMA((7,)),
            ],
            compiler_params=pltpu.CompilerParams(
                collective_id=0, has_side_effects=True, vmem_limit_bytes=60 * 1024 * 1024),
            name="gmlp",
        )(act_in, row(ln1_scale), row(ln1_bias), w_in, row(b_in), row(ln2_scale), row(ln2_bias),
          w_spatial, row(b_spatial), causal_mask, w_out, row(b_out))

    return jax.shard_map(local_block, mesh=mesh, in_specs=(row_spec,) + (P(),) * 11, out_specs=row_spec, check_vma=False)
```

```python
import functools

import jax
import jax.numpy as jnp
from jax import lax
from jax.experimental import pallas as pl
from jax.experimental.pallas import tpu as pltpu
from jax.sharding import PartitionSpec as P

LN_EPS = 1e-6
GELU_A = 0.7978845608028654
GELU_B = GELU_A * 0.044715
COLS = 512
LANES = 128
MESH = pl.DeviceIdType.MESH
F32 = jnp.float32
BF16 = jnp.bfloat16


def gelu(a):
    return a * jax.nn.sigmoid(a * (2 * GELU_A + 2 * GELU_B * (a * a)))


def layer_norm(x, gain, shift):
    width = x.shape[-1]
    mean = jnp.sum(x, axis=-1, keepdims=True) * (1.0 / width)
    centered = x - mean
    var = jnp.sum(centered * centered, axis=-1, keepdims=True) * (1.0 / width)
    return centered * lax.rsqrt(var + LN_EPS) * gain + shift


def wide(ref, tiles, *where):
    return jnp.concatenate([ref[(j, *where)] for j in tiles], axis=1)


def body(n, act, ln1s_hbm, ln1b_hbm, w_in, b_in_hbm, ln2s_hbm, ln2b_hbm, w_sp, b_sp_hbm, mask, w_out, b_out_hbm, out,
         ln1s, ln1b, b_in, ln2s, ln2b, b_sp, b_out, xbuf, wi, wo, ws, mk, vn, g, u, q, ybuf, bias, stat,
         xs_sem, xr_sem, ys_sem, yr_sem, wi_sem, wo_sem, ws_sem, mk_sem, vec_sem):
    me = lax.axis_index("seq")
    chip, core = me // 2, lax.rem(me, 2)
    partner = chip * 2 + 1 - core
    far = (1 - chip) * 2
    early0 = (1 - chip) * core
    late0 = (1 - chip) * (1 - core)
    rows, width = act.shape[1], act.shape[2]
    length = n * rows
    half = rows // 2
    gate = w_out.shape[0]
    gate_tiles = gate // LANES
    n_cols = gate // COLS
    per = COLS // LANES

    def lanes(j):
        return pl.ds(j * LANES, LANES)

    def wi_copy(j):
        return pltpu.make_async_copy(w_in.at[:, lanes(j)], wi.at[j], wi_sem.at[j])

    def ws_copy(j):
        return pltpu.make_async_copy(w_sp.at[:, lanes(j)], ws.at[j], ws_sem.at[j])

    def wo_copy(j):
        return pltpu.make_async_copy(w_out.at[:, lanes(j)], wo.at[j], wo_sem.at[j])

    def mk_copy():
        return pltpu.make_async_copy(mask, mk, mk_sem)

    def own_x(p):
        part = pl.ds(p * half, half)
        return pltpu.make_async_copy(act.at[me, part], xbuf.at[me, part], xr_sem.at[me, p])

    def x_send(dest, p):
        part = pl.ds(p * half, half)
        return pltpu.make_async_remote_copy(
            src_ref=act.at[dest, part], dst_ref=xbuf.at[me, part], send_sem=xs_sem.at[dest, p], recv_sem=xr_sem.at[me, p],
            device_id={"seq": dest}, device_id_type=MESH)

    def x_recv(block, p):
        part = pl.ds(p * half, half)
        return pltpu.make_async_remote_copy(
            src_ref=act.at[partner, part], dst_ref=xbuf.at[block, part], send_sem=xs_sem.at[block, p],
            recv_sem=xr_sem.at[block, p], device_id={"seq": partner}, device_id_type=MESH)

    def extra_own(p):
        part = pl.ds(p * half, half)
        return pltpu.make_async_copy(act.at[far, part], xbuf.at[n, part], xr_sem.at[n, p])

    def extra_send(p):
        part = pl.ds(p * half, half)
        return pltpu.make_async_remote_copy(
            src_ref=act.at[far + 1, part], dst_ref=xbuf.at[n, part], send_sem=xs_sem.at[n, p], recv_sem=xr_sem.at[n, p],
            device_id={"seq": partner}, device_id_type=MESH)

    def y_send(slot):
        extra = slot // n
        seq = (1 - extra) * me + extra * (far + core)
        return pltpu.make_async_remote_copy(
            src_ref=ybuf.at[slot], dst_ref=out.at[seq], send_sem=ys_sem.at[slot], recv_sem=yr_sem.at[seq],
            device_id={"seq": slot - extra * n}, device_id_type=MESH)

    def y_recv(block):
        return pltpu.make_async_remote_copy(
            src_ref=ybuf.at[block], dst_ref=out.at[block], send_sem=ys_sem.at[block], recv_sem=yr_sem.at[block],
            device_id={"seq": block}, device_id_type=MESH)

    def y_own(slot):
        extra = slot // n
        seq = (1 - extra) * me + extra * (far + core)
        return pltpu.make_async_copy(ybuf.at[slot], out.at[seq], yr_sem.at[seq])

    vectors = [pltpu.make_async_copy(src, dst, vec_sem.at[k]) for k, (src, dst) in enumerate((
        (ln1s_hbm, ln1s), (ln1b_hbm, ln1b), (b_sp_hbm, b_sp), (b_in_hbm, b_in), (ln2s_hbm, ln2s), (ln2b_hbm, ln2b),
        (b_out_hbm, b_out)))]

    barrier = pltpu.get_barrier_semaphore()
    for k in range(1, n):
        pl.semaphore_signal(barrier, inc=1, device_id={"seq": lax.rem(me + k, n)}, device_id_type=MESH)
    for p in range(2):
        own_x(p).start()
    for copy in vectors:
        copy.start()
    for j in range(2 * gate_tiles):
        wi_copy((j + gate_tiles) % (2 * gate_tiles)).start()
    pl.semaphore_wait(barrier, n - 1)
    for dest in (far + chip, partner, far + 1 - chip):
        for p in range(2):
            x_send(dest, p).start()
    @pl.when(me == 0)
    def _():
        for p in range(2):
            extra_send(p).start()
            extra_own(p).start()

    for j in range(length // LANES):
        ws_copy(j).start()
    mk_copy().start()
    for j in range(width // LANES):
        wo_copy(j).start()

    for copy in vectors:
        copy.wait()
    for i in range(n):
        at = pl.ds(i * rows, rows)
        bias[at, :] = jnp.broadcast_to(b_sp[:, at], (LANES, rows)).T

    def stage_a(t, first):
        if first:
            pieces = [(me, 0), (me, 1)]
            for p in range(2):
                own_x(p).wait()
        else:
            near, extra = 1 - (t + 2) // 4, t // 4
            remote = 1 - near - extra
            side = t - 2
            pieces = [
                (near * partner + remote * (far + early0 * side) + extra * n, remote * (1 - early0) * side),
                (near * partner + remote * (far + early0 * side + (1 - early0)) + extra * n,
                 near + extra + remote * (early0 + (1 - early0) * side))]

            @pl.when(extra * (1 - core) == 1)
            def _():
                for p in range(2):
                    extra_own(p).wait()

            @pl.when(extra * (1 - core) == 0)
            def _():
                for block, p in pieces:
                    x_recv(block, p).wait_recv()

        starts = [pl.multiple_of(lax.rem(block, n) * rows + p * half, half) for block, p in pieces]
        step1 = 64
        for k, (block, p) in enumerate(pieces):
            for r in range(half // step1):
                x = xbuf[block, pl.ds(pl.multiple_of(p * half, half) + r * step1, step1), :].astype(F32)
                x = layer_norm(x, ln1s[...], ln1b[...]).astype(BF16)
                for j in range(width // LANES):
                    u[j, pl.ds(k * half + r * step1, step1), :] = x[:, j * LANES:(j + 1) * LANES]

        def chunk(c):
            tiles = range(c * per, (c + 1) * per)
            acc = jnp.dot(wide(u, range(width // LANES)), wide(wi, tiles), preferred_element_type=F32)
            return gelu(acc + b_in[:, pl.ds(c * COLS, COLS)]).astype(BF16), jnp.minimum(jnp.abs(acc[:, :LANES]), 0.0)

        def put(dst, c, value):
            for j in range(per):
                for k in range(2):
                    dst[c * per + j, pl.ds(starts[k], half), :] = value[k * half:(k + 1) * half, j * LANES:(j + 1) * LANES]

        if first:
            for j in range(gate_tiles, 2 * gate_tiles):
                wi_copy(j).wait()
        for c in range(n_cols):
            value, _ = chunk(n_cols + c)
            put(vn, c, value)
            value = value.astype(F32)
            tiles = [value[:, j * LANES:(j + 1) * LANES] for j in range(per)]
            if c == 0:
                pivot = tiles[0]
                stat[0] = pivot
                tiles = tiles[1:]
            else:
                pivot = stat[0]
            diffs = [v - pivot for v in tiles]
            total = sum(diffs[1:], diffs[0])
            squares = sum([d * d for d in diffs[1:]], diffs[0] * diffs[0])
            stat[1] = total if c == 0 else stat[1] + total
            stat[2] = squares if c == 0 else stat[2] + squares
        if first:
            for j in range(gate_tiles):
                wi_copy(j).wait()
        total = stat[1]
        mean_lane = stat[0] + total * (1.0 / gate_tiles)
        mean = jnp.sum(mean_lane, axis=-1, keepdims=True) * (1.0 / LANES)
        away = mean_lane - mean
        spread = (stat[2] - total * total * (1.0 / gate_tiles)) + gate_tiles * (away * away)
        var = jnp.maximum(jnp.sum(spread, axis=-1, keepdims=True) * (1.0 / gate), 0.0)
        stat[0] = jnp.broadcast_to(mean, (rows, LANES))
        stat[1] = jnp.broadcast_to(lax.rsqrt(var + LN_EPS), (rows, LANES))

        def norm(j, mean_now):
            for k in range(2):
                part = pl.ds(starts[k], half)
                here = pl.ds(k * half, half)
                value = (vn[j, part, :].astype(F32) - mean_now[k * half:(k + 1) * half]) * stat[1, here]
                vn[j, part, :] = (value * ln2s[:, lanes(j)] + ln2b[:, lanes(j)]).astype(BF16)

        for c in range(n_cols):
            value, zero = chunk(c)
            put(g, c, value)
            mean_now = stat[0] + zero
            for j in range(c * per, (c + 1) * per):
                norm(j, mean_now)

    def stage_b(slot, i):
        at = pl.ds(i * rows, rows)
        depth = (i + 1) * rows
        for j in range(depth // LANES):
            ws[j, at, :] = jnp.where(mk[at, lanes(j)] > 0, ws[j, at, :].astype(F32), 0.0).astype(BF16)
        for c in range(n_cols):
            tiles = range(c * per, (c + 1) * per)
            s = jnp.dot(wide(ws, range(depth // LANES), at), wide(vn, tiles, pl.ds(0, depth)), preferred_element_type=F32)
            for j in range(per):
                t = (s[:, j * LANES:(j + 1) * LANES] + bias[at, :]).astype(BF16).astype(F32)
                q[tiles[j]] = (g[tiles[j], at, :].astype(F32) * t).astype(BF16)
        for c in range(width // COLS):
            cols = pl.ds(c * COLS, COLS)
            y = jnp.dot(wide(q, range(gate_tiles)), wide(wo, range(c * per, (c + 1) * per)), preferred_element_type=F32)
            ybuf[slot, :, cols] = (xbuf[slot, :, cols].astype(F32) + (y + b_out[:, cols])).astype(BF16)

    stage_a(0, True)

    def outer(k, carry):
        last = k // n
        def upto(k):
            return (early0 * (3 + (k + 3) // 4 + k // 4) + late0 * (2 + 2 * ((k + 2) // 4) + k // 4) + chip * n)

        def one(t, c):
            stage_a(t, False)
            return c

        lax.fori_loop(jnp.where(k == 0, 1, upto(k - 1)), upto(k), one, 0)

        @pl.when(k == 0)
        def _():
            for j in range(length // LANES):
                ws_copy(j).wait()
            mk_copy().wait()
            for j in range(width // LANES):
                wo_copy(j).wait()

        slot = early0 * ((1 - last) * lax.rem(k + 2, n) + last * n) + late0 * k + chip * (k + 1)
        block = lax.rem(slot, n)
        for i in range(n):
            pl.when(block == i)(functools.partial(stage_b, slot, i))

        @pl.when(me == block)
        def _():
            y_own(slot).start()

        @pl.when(me != block)
        def _():
            y_send(slot).start()

        return carry

    lax.fori_loop(0, (1 - chip) * (n + 1) + chip * (n - 1), outer, 0)

    for k in range(1, n):
        for p in range(2):
            x_send(lax.rem(me + k, n), p).wait_send()

    @pl.when(me == 0)
    def _():
        for p in range(2):
            extra_send(p).wait_send()
        y_own(n).wait()

    @pl.when(me == 1)
    def _():
        y_send(n).wait_send()

    @pl.when((me != 0) & (chip == 0))
    def _():
        y_send(0).wait_send()

    for block in range(1, n):
        @pl.when(me != block)
        def _():
            y_send(block).wait_send()

    for seq in range(n):
        @pl.when((me != seq) & ((me != 0) | (seq != 2)))
        def _():
            y_recv(seq).wait_recv()

    y_own(me).wait()


def write_out(src, dst, sem):
    copies = [pltpu.make_async_copy(src.at[i], dst.at[i], sem.at[i]) for i in range(src.shape[0])]
    for copy in copies:
        copy.start()
    for copy in copies:
        copy.wait()


def solution(mesh):
    n = mesh.shape["seq"]
    row_spec = P("data", "seq", None)

    def local_block(act_in, ln1_scale, ln1_bias, w_in, b_in, ln2_scale, ln2_bias, w_spatial, b_spatial, causal_mask, w_out, b_out):
        rows, width = act_in.shape[1:]
        length = n * rows
        gate = w_out.shape[0]
        hbm = pl.BlockSpec(memory_space=pl.ANY)

        def row(v):
            return v.reshape(1, -1)

        result = pl.pallas_call(
            functools.partial(body, n),
            out_shape=pltpu.VMEM(act_in.shape, act_in.dtype),
            in_specs=[hbm] * 12,
            out_specs=hbm,
            scratch_shapes=[
                pltpu.VMEM((1, width), F32),
                pltpu.VMEM((1, width), F32),
                pltpu.VMEM((1, 2 * gate), F32),
                pltpu.VMEM((1, gate), F32),
                pltpu.VMEM((1, gate), F32),
                pltpu.VMEM((1, length), F32),
                pltpu.VMEM((1, width), F32),
                pltpu.VMEM((n + 1, rows, width), BF16),
                pltpu.VMEM((2 * gate // LANES, width, LANES), BF16),
                pltpu.VMEM((width // LANES, gate, LANES), BF16),
                pltpu.VMEM((length // LANES, length, LANES), BF16),
                pltpu.VMEM((length, length), jnp.int32),
                pltpu.VMEM((gate // LANES, length, LANES), BF16),
                pltpu.VMEM((gate // LANES, length, LANES), BF16),
                pltpu.VMEM((width // LANES, rows, LANES), BF16),
                pltpu.VMEM((gate // LANES, rows, LANES), BF16),
                pltpu.VMEM((n + 1, rows, width), BF16),
                pltpu.VMEM((length, LANES), F32),
                pltpu.VMEM((3, rows, LANES), F32),
                pltpu.SemaphoreType.DMA((n + 1, 2)),
                pltpu.SemaphoreType.DMA((n + 1, 2)),
                pltpu.SemaphoreType.DMA((n + 1,)),
                pltpu.SemaphoreType.DMA((n,)),
                pltpu.SemaphoreType.DMA((2 * gate // LANES,)),
                pltpu.SemaphoreType.DMA((width // LANES,)),
                pltpu.SemaphoreType.DMA((length // LANES,)),
                pltpu.SemaphoreType.DMA,
                pltpu.SemaphoreType.DMA((7,)),
            ],
            compiler_params=pltpu.CompilerParams(
                collective_id=0, has_side_effects=True, vmem_limit_bytes=60 * 1024 * 1024),
            name="gmlp",
        )(act_in, row(ln1_scale), row(ln1_bias), w_in, row(b_in), row(ln2_scale), row(ln2_bias),
          w_spatial, row(b_spatial), causal_mask, w_out, row(b_out))
        return pl.pallas_call(
            write_out,
            out_shape=jax.ShapeDtypeStruct(act_in.shape, act_in.dtype),
            in_specs=[pl.BlockSpec(memory_space=pltpu.VMEM)],
            out_specs=hbm,
            scratch_shapes=[pltpu.SemaphoreType.DMA((act_in.shape[0],))],
            compiler_params=pltpu.CompilerParams(vmem_limit_bytes=1024 * 1024),
            name="write_out",
        )(result)

    return jax.shard_map(local_block, mesh=mesh, in_specs=(row_spec,) + (P(),) * 11, out_specs=row_spec, check_vma=False)
```

```python
import functools

import jax
import jax.numpy as jnp
from jax import lax
from jax.experimental import pallas as pl
from jax.experimental.pallas import tpu as pltpu
from jax.sharding import PartitionSpec as P

LN_EPS = 1e-6
GELU_A = 0.7978845608028654
GELU_B = GELU_A * 0.044715
COLS = 512
LANES = 128
MESH = pl.DeviceIdType.MESH
F32 = jnp.float32
BF16 = jnp.bfloat16


def gelu(a):
    return a * jax.nn.sigmoid(a * (2 * GELU_A + 2 * GELU_B * (a * a)))


def layer_norm(x, gain, shift):
    width = x.shape[-1]
    mean = jnp.sum(x, axis=-1, keepdims=True) * (1.0 / width)
    centered = x - mean
    var = jnp.sum(centered * centered, axis=-1, keepdims=True) * (1.0 / width)
    return centered * lax.rsqrt(var + LN_EPS) * gain + shift


def wide(ref, tiles, *where):
    return jnp.concatenate([ref[(j, *where)] for j in tiles], axis=1)


def body(n, act, ln1s_hbm, ln1b_hbm, w_in, b_in_hbm, ln2s_hbm, ln2b_hbm, w_sp, b_sp_hbm, mask, w_out, b_out_hbm, out,
         ln1s, ln1b, b_in, ln2s, ln2b, b_sp, b_out, xbuf, wi, wo, ws, mk, vn, g, u, q, ybuf, bias, stat,
         xs_sem, xr_sem, ys_sem, yr_sem, wi_sem, wo_sem, ws_sem, mk_sem, vec_sem):
    me = lax.axis_index("seq")
    chip, core = me // 2, lax.rem(me, 2)
    partner = chip * 2 + 1 - core
    far = (1 - chip) * 2
    early0 = (1 - chip) * core
    late0 = (1 - chip) * (1 - core)
    rows, width = act.shape[1], act.shape[2]
    length = n * rows
    half = rows // 2
    gate = w_out.shape[0]
    gate_tiles = gate // LANES
    n_cols = gate // COLS
    per = COLS // LANES

    def lanes(j):
        return pl.ds(j * LANES, LANES)

    def wi_copy(j):
        return pltpu.make_async_copy(w_in.at[:, lanes(j)], wi.at[j], wi_sem.at[j])

    def ws_copy(j):
        return pltpu.make_async_copy(w_sp.at[:, lanes(j)], ws.at[j], ws_sem.at[j])

    def wo_copy(j):
        return pltpu.make_async_copy(w_out.at[:, lanes(j)], wo.at[j], wo_sem.at[j])

    def mk_copy():
        return pltpu.make_async_copy(mask, mk, mk_sem)

    def own_x(p):
        part = pl.ds(p * half, half)
        return pltpu.make_async_copy(act.at[me, part], xbuf.at[me, part], xr_sem.at[me, p])

    def x_send(dest, p):
        part = pl.ds(p * half, half)
        return pltpu.make_async_remote_copy(
            src_ref=act.at[dest, part], dst_ref=xbuf.at[me, part], send_sem=xs_sem.at[dest, p], recv_sem=xr_sem.at[me, p],
            device_id={"seq": dest}, device_id_type=MESH)

    def x_recv(block, p):
        part = pl.ds(p * half, half)
        return pltpu.make_async_remote_copy(
            src_ref=act.at[partner, part], dst_ref=xbuf.at[block, part], send_sem=xs_sem.at[block, p],
            recv_sem=xr_sem.at[block, p], device_id={"seq": partner}, device_id_type=MESH)

    def extra_own(p):
        part = pl.ds(p * half, half)
        return pltpu.make_async_copy(act.at[far, part], xbuf.at[n, part], xr_sem.at[n, p])

    def extra_send(p):
        part = pl.ds(p * half, half)
        return pltpu.make_async_remote_copy(
            src_ref=act.at[far + 1, part], dst_ref=xbuf.at[n, part], send_sem=xs_sem.at[n, p], recv_sem=xr_sem.at[n, p],
            device_id={"seq": partner}, device_id_type=MESH)

    def y_send(slot):
        extra = slot // n
        seq = (1 - extra) * me + extra * (far + core)
        return pltpu.make_async_remote_copy(
            src_ref=ybuf.at[slot], dst_ref=out.at[seq], send_sem=ys_sem.at[slot], recv_sem=yr_sem.at[seq],
            device_id={"seq": slot - extra * n}, device_id_type=MESH)

    def y_recv(block):
        return pltpu.make_async_remote_copy(
            src_ref=ybuf.at[block], dst_ref=out.at[block], send_sem=ys_sem.at[block], recv_sem=yr_sem.at[block],
            device_id={"seq": block}, device_id_type=MESH)

    def y_own(slot):
        extra = slot // n
        seq = (1 - extra) * me + extra * (far + core)
        return pltpu.make_async_copy(ybuf.at[slot], out.at[seq], yr_sem.at[seq])

    vectors = [pltpu.make_async_copy(src, dst, vec_sem.at[k]) for k, (src, dst) in enumerate((
        (ln1s_hbm, ln1s), (ln1b_hbm, ln1b), (b_sp_hbm, b_sp), (b_in_hbm, b_in), (ln2s_hbm, ln2s), (ln2b_hbm, ln2b),
        (b_out_hbm, b_out)))]

    barrier = pltpu.get_barrier_semaphore()
    for peer in (far + chip, far + 1 - chip, partner):
        pl.semaphore_signal(barrier, inc=1, device_id={"seq": peer}, device_id_type=MESH)
    for p in range(2):
        own_x(p).start()
    for copy in vectors:
        copy.start()
    for j in range(2 * gate_tiles):
        wi_copy((j + gate_tiles) % (2 * gate_tiles)).start()
    pl.semaphore_wait(barrier, n - 1)
    for dest in (far + chip, partner, far + 1 - chip):
        for p in range(2):
            x_send(dest, p).start()
    @pl.when(me == 0)
    def _():
        for p in range(2):
            extra_send(p).start()
            extra_own(p).start()

    for j in range(length // LANES):
        ws_copy(j).start()
    mk_copy().start()
    for j in range(width // LANES):
        wo_copy(j).start()

    for copy in vectors:
        copy.wait()
    for i in range(n):
        at = pl.ds(i * rows, rows)
        bias[at, :] = jnp.broadcast_to(b_sp[:, at], (LANES, rows)).T

    def stage_a(t, first):
        if first:
            pieces = [(me, 0), (me, 1)]
            for p in range(2):
                own_x(p).wait()
        else:
            near, extra = 1 - (t + 2) // 4, t // 4
            remote = 1 - near - extra
            side = t - 2
            pieces = [
                (near * partner + remote * (far + early0 * side) + extra * n, remote * (1 - early0) * side),
                (near * partner + remote * (far + early0 * side + (1 - early0)) + extra * n,
                 near + extra + remote * (early0 + (1 - early0) * side))]

            @pl.when(extra * (1 - core) == 1)
            def _():
                for p in range(2):
                    extra_own(p).wait()

            @pl.when(extra * (1 - core) == 0)
            def _():
                for block, p in pieces:
                    x_recv(block, p).wait_recv()

        starts = [pl.multiple_of(lax.rem(block, n) * rows + p * half, half) for block, p in pieces]
        step1 = 64
        for k, (block, p) in enumerate(pieces):
            for r in range(half // step1):
                x = xbuf[block, pl.ds(pl.multiple_of(p * half, half) + r * step1, step1), :].astype(F32)
                x = layer_norm(x, ln1s[...], ln1b[...]).astype(BF16)
                for j in range(width // LANES):
                    u[j, pl.ds(k * half + r * step1, step1), :] = x[:, j * LANES:(j + 1) * LANES]

        def chunk(c):
            tiles = range(c * per, (c + 1) * per)
            acc = jnp.dot(wide(u, range(width // LANES)), wide(wi, tiles), preferred_element_type=F32)
            return gelu(acc + b_in[:, pl.ds(c * COLS, COLS)]).astype(BF16), jnp.minimum(jnp.abs(acc[:, :LANES]), 0.0)

        def put(dst, c, value):
            for j in range(per):
                for k in range(2):
                    dst[c * per + j, pl.ds(starts[k], half), :] = value[k * half:(k + 1) * half, j * LANES:(j + 1) * LANES]

        if first:
            for j in range(gate_tiles, 2 * gate_tiles):
                wi_copy(j).wait()
        for c in range(n_cols):
            value, _ = chunk(n_cols + c)
            put(vn, c, value)
            value = value.astype(F32)
            tiles = [value[:, j * LANES:(j + 1) * LANES] for j in range(per)]
            if c == 0:
                pivot = tiles[0]
                stat[0] = pivot
                tiles = tiles[1:]
            else:
                pivot = stat[0]
            diffs = [v - pivot for v in tiles]
            total = sum(diffs[1:], diffs[0])
            squares = sum([d * d for d in diffs[1:]], diffs[0] * diffs[0])
            stat[1] = total if c == 0 else stat[1] + total
            stat[2] = squares if c == 0 else stat[2] + squares
        if first:
            for j in range(gate_tiles):
                wi_copy(j).wait()
        total = stat[1]
        mean_lane = stat[0] + total * (1.0 / gate_tiles)
        mean = jnp.sum(mean_lane, axis=-1, keepdims=True) * (1.0 / LANES)
        away = mean_lane - mean
        spread = (stat[2] - total * total * (1.0 / gate_tiles)) + gate_tiles * (away * away)
        var = jnp.maximum(jnp.sum(spread, axis=-1, keepdims=True) * (1.0 / gate), 0.0)
        stat[0] = jnp.broadcast_to(mean, (rows, LANES))
        stat[1] = jnp.broadcast_to(lax.rsqrt(var + LN_EPS), (rows, LANES))

        def norm(j, mean_now):
            for k in range(2):
                part = pl.ds(starts[k], half)
                here = pl.ds(k * half, half)
                value = (vn[j, part, :].astype(F32) - mean_now[k * half:(k + 1) * half]) * stat[1, here]
                vn[j, part, :] = (value * ln2s[:, lanes(j)] + ln2b[:, lanes(j)]).astype(BF16)

        for c in range(n_cols):
            value, zero = chunk(c)
            put(g, c, value)
            mean_now = stat[0] + zero
            for j in range(c * per, (c + 1) * per):
                norm(j, mean_now)

    def stage_b(slot, i):
        at = pl.ds(i * rows, rows)
        depth = (i + 1) * rows
        for j in range(depth // LANES):
            ws[j, at, :] = jnp.where(mk[at, lanes(j)] > 0, ws[j, at, :].astype(F32), 0.0).astype(BF16)
        for c in range(n_cols):
            tiles = range(c * per, (c + 1) * per)
            s = jnp.dot(wide(ws, range(depth // LANES), at), wide(vn, tiles, pl.ds(0, depth)), preferred_element_type=F32)
            for j in range(per):
                t = (s[:, j * LANES:(j + 1) * LANES] + bias[at, :]).astype(BF16).astype(F32)
                q[tiles[j]] = (g[tiles[j], at, :].astype(F32) * t).astype(BF16)
        for c in range(width // COLS):
            cols = pl.ds(c * COLS, COLS)
            y = jnp.dot(wide(q, range(gate_tiles)), wide(wo, range(c * per, (c + 1) * per)), preferred_element_type=F32)
            ybuf[slot, :, cols] = (xbuf[slot, :, cols].astype(F32) + (y + b_out[:, cols])).astype(BF16)

    stage_a(0, True)

    def outer(k, carry):
        last = k // n
        def upto(k):
            return (early0 * (3 + (k + 3) // 4 + k // 4) + late0 * (2 + 2 * ((k + 2) // 4) + k // 4) + chip * n)

        def one(t, c):
            stage_a(t, False)
            return c

        lax.fori_loop(jnp.where(k == 0, 1, upto(k - 1)), upto(k), one, 0)

        @pl.when(k == 0)
        def _():
            for j in range(length // LANES):
                ws_copy(j).wait()
            mk_copy().wait()
            for j in range(width // LANES):
                wo_copy(j).wait()

        slot = early0 * ((1 - last) * lax.rem(k + 2, n) + last * n) + late0 * k + chip * (k + 1)
        block = lax.rem(slot, n)
        for i in range(n):
            pl.when(block == i)(functools.partial(stage_b, slot, i))

        @pl.when(me == block)
        def _():
            y_own(slot).start()

        @pl.when(me != block)
        def _():
            y_send(slot).start()

        return carry

    lax.fori_loop(0, (1 - chip) * (n + 1) + chip * (n - 1), outer, 0)

    for k in range(1, n):
        for p in range(2):
            x_send(lax.rem(me + k, n), p).wait_send()

    @pl.when(me == 0)
    def _():
        for p in range(2):
            extra_send(p).wait_send()
        y_own(n).wait()

    @pl.when(me == 1)
    def _():
        y_send(n).wait_send()

    @pl.when((me != 0) & (chip == 0))
    def _():
        y_send(0).wait_send()

    for block in range(1, n):
        @pl.when(me != block)
        def _():
            y_send(block).wait_send()

    for seq in range(n):
        @pl.when((me != seq) & ((me != 0) | (seq != 2)))
        def _():
            y_recv(seq).wait_recv()

    y_own(me).wait()


def solution(mesh):
    n = mesh.shape["seq"]
    row_spec = P("data", "seq", None)

    def local_block(act_in, ln1_scale, ln1_bias, w_in, b_in, ln2_scale, ln2_bias, w_spatial, b_spatial, causal_mask, w_out, b_out):
        rows, width = act_in.shape[1:]
        length = n * rows
        gate = w_out.shape[0]
        hbm = pl.BlockSpec(memory_space=pl.ANY)

        def row(v):
            return v.reshape(1, -1)

        return pl.pallas_call(
            functools.partial(body, n),
            out_shape=pltpu.VMEM(act_in.shape, act_in.dtype),
            in_specs=[hbm] * 12,
            out_specs=hbm,
            scratch_shapes=[
                pltpu.VMEM((1, width), F32),
                pltpu.VMEM((1, width), F32),
                pltpu.VMEM((1, 2 * gate), F32),
                pltpu.VMEM((1, gate), F32),
                pltpu.VMEM((1, gate), F32),
                pltpu.VMEM((1, length), F32),
                pltpu.VMEM((1, width), F32),
                pltpu.VMEM((n + 1, rows, width), BF16),
                pltpu.VMEM((2 * gate // LANES, width, LANES), BF16),
                pltpu.VMEM((width // LANES, gate, LANES), BF16),
                pltpu.VMEM((length // LANES, length, LANES), BF16),
                pltpu.VMEM((length, length), jnp.int32),
                pltpu.VMEM((gate // LANES, length, LANES), BF16),
                pltpu.VMEM((gate // LANES, length, LANES), BF16),
                pltpu.VMEM((width // LANES, rows, LANES), BF16),
                pltpu.VMEM((gate // LANES, rows, LANES), BF16),
                pltpu.VMEM((n + 1, rows, width), BF16),
                pltpu.VMEM((length, LANES), F32),
                pltpu.VMEM((3, rows, LANES), F32),
                pltpu.SemaphoreType.DMA((n + 1, 2)),
                pltpu.SemaphoreType.DMA((n + 1, 2)),
                pltpu.SemaphoreType.DMA((n + 1,)),
                pltpu.SemaphoreType.DMA((n,)),
                pltpu.SemaphoreType.DMA((2 * gate // LANES,)),
                pltpu.SemaphoreType.DMA((width // LANES,)),
                pltpu.SemaphoreType.DMA((length // LANES,)),
                pltpu.SemaphoreType.DMA,
                pltpu.SemaphoreType.DMA((7,)),
            ],
            compiler_params=pltpu.CompilerParams(
                collective_id=0, has_side_effects=True, vmem_limit_bytes=60 * 1024 * 1024),
            name="gmlp",
        )(act_in, row(ln1_scale), row(ln1_bias), w_in, row(b_in), row(ln2_scale), row(ln2_bias),
          w_spatial, row(b_spatial), causal_mask, w_out, row(b_out))

    return jax.shard_map(local_block, mesh=mesh, in_specs=(row_spec,) + (P(),) * 11, out_specs=row_spec, check_vma=False)
```
